32 devices in a mesh: groups: 2 (over y), gx: 4 (over z), gy: 2 (over x), gz: 2 (over core).
Axes of the slice: x: 2, y: 2, z: 4, core: 2. Of those that a mesh axis runs over, the one named last changes fastest.
Arguments:
- coords: float32 [8, 8, 16, 3, 128], P(('groups', 'gx'), 'gy', 'gz'), parts along dimension 0, may hold values from 0 to 1.1
- charges: float32 [8, 8, 16, 128], P(('groups', 'gx'), 'gy', 'gz'), parts along dimension 0, may hold values from -2 to 2
- atom_types: int32 [8, 8, 16, 128], P(('groups', 'gx'), 'gy', 'gz'), parts along dimension 0, may hold values from 0 to 63
- counts: int32 [8, 8, 16], P(('groups', 'gx'), 'gy', 'gz'), parts along dimension 0, may hold values from 64 to 128
- c6_table: float32 [64, 64], replicated, may hold values from 0.0001 to 0.001
- c12_table: float32 [64, 64], replicated, may hold values from 1e-08 to 1e-07
Outputs:
- forces: float32 [8, 8, 16, 3, 128], P(('groups', 'gx'), 'gy', 'gz'), parts along dimension 0
- energy: float32 [2], P('groups'), parts along dimension 0
The draws below stay inside these ranges and needn't reach their ends.
There are 2 independent parts, one for each index of `groups`. The reference program is written for one: setup_inputs(seed, part) draws one part's arguments, and reference() takes and returns one part's arrays. A program takes and returns all parts, laid end to end along the dimension named above; an argument that names none is the same for every part. Nothing has to cross between parts.
All inputs are finite; a program needn't handle non-finite values.
Results may differ from the reference program's by a relative error of at most 0.0003.
Values sent between devices are 32-bit elements; how exact they have to be, the bound alone decides.
A program may use at most 64 MiB of HBM per device.

```python
import math
import jax
import jax.numpy as jnp
from jax import lax

SLOTS = 128
TYPES = 64
NX = 4
NY = 8
NZ = 16


def set_ends(result, stream_key, low, top_value):
    index_at = [jax.random.randint(jax.random.fold_in(stream_key, axis), (), 0, length) for axis, length in enumerate(result.shape)]
    widest = result.shape.index(max(result.shape))
    beside = index_at[:widest] + [(index_at[widest] + 1) % result.shape[widest]] + index_at[widest + 1:]
    return result.at[tuple(index_at)].set(low).at[tuple(beside)].set(top_value)


def steps_of(key, extent, cuts, least, top_value):
    factor_of = 1.0
    for position, blocks in cuts:
        draws = jax.random.uniform(jax.random.fold_in(jax.random.fold_in(key, 6), position), (blocks,), jnp.float32, least / len(cuts), top_value / len(cuts))
        factor_of = factor_of * jnp.repeat(jnp.exp(draws), extent[position] // blocks).reshape((-1,) + (1,) * (len(extent) - 1 - position))
    return factor_of


def bell_draw(own_key, dims, scale, reach, split=(), kind=jnp.bfloat16):
    level = steps_of(own_key, dims, split, -0.22, 0.18) if split else 1.0
    result = jax.random.normal(own_key, dims, jnp.float32) * scale * level
    return jnp.minimum(jnp.maximum(result, -reach), reach).astype(kind)


def setup_inputs(seed: int = 0, part: int = 0) -> dict:
    streams_of = jax.random.split(jax.random.key(seed), 7)
    own_keys = jax.random.split(jax.random.fold_in(streams_of[6], part), 7)
    return {
        "coords": jnp.clip(1.1 * jax.random.uniform(own_keys[0], (NX, NY, NZ, 3, SLOTS), jnp.float32) ** steps_of(own_keys[0], (NX, NY, NZ, 3, SLOTS), ((0, 4), (1, 2), (2, 2)), -0.2, 0.2), 0.0, 1.1),
        "charges": bell_draw(own_keys[1], (NX, NY, NZ, SLOTS), 0.4, 2.0, ((0, 4), (1, 2), (2, 2)), jnp.float32),
        "atom_types": set_ends(jax.random.randint(own_keys[2], (NX, NY, NZ, SLOTS), 0, TYPES), jax.random.fold_in(own_keys[2], 1), 0, TYPES - 1).astype(jnp.int32),
        "counts": set_ends(jax.random.randint(own_keys[3], (NX, NY, NZ), SLOTS // 2, SLOTS + 1), jax.random.fold_in(own_keys[3], 1), SLOTS // 2, SLOTS).astype(jnp.int32),
        "c6_table": jnp.clip(jnp.exp(jax.random.uniform(streams_of[4], (TYPES, TYPES), jnp.float32, math.log(0.0001), math.log(0.001))), 0.0001, 0.001),
        "c12_table": jnp.clip(jnp.exp(jax.random.uniform(streams_of[5], (TYPES, TYPES), jnp.float32, math.log(9.99999993922529e-09), math.log(1.0000000116860974e-07))), 9.99999993922529e-09, 1.0000000116860974e-07),
    }


CELL_EDGE = 1.1
CUT_SQUARE = 1.0
SOFTEN = 0.09
ENERGY_UNIT = 0.1
CELL_PAIRS = ((0, 1), (0, 2), (0, 3), (0, 4), (0, 5), (0, 6), (0, 7), (1, 2), (1, 4), (2, 4), (1, 6), (2, 5), (4, 3))

def corner_bits(corner_index):
    return (corner_index >> 2 & 1, corner_index >> 1 & 1, corner_index & 1)

def pack_cells(coords, charges, atom_types, counts):
    slot_count = coords.shape[-1]
    occupied = (jnp.arange(slot_count, dtype=jnp.int32) < counts[..., None]).astype(jnp.float32)
    return jnp.concatenate([coords, charges[..., None, :], atom_types.astype(jnp.float32)[..., None, :], occupied[..., None, :]], axis=3)

def tile_terms(pack_a, pack_b, c6_sym, c12_sym, offset, pair_mask):
    type_ids = jnp.arange(c6_sym.shape[0]).astype(jnp.float32)
    type_hot_a = (pack_a[4][:, None] == type_ids[None, :]).astype(jnp.float32)
    type_hot_b = (pack_b[4][:, None] == type_ids[None, :]).astype(jnp.float32)
    c6_pair = jnp.dot(jnp.dot(type_hot_a, c6_sym, precision=lax.Precision.HIGHEST), type_hot_b.T, precision=lax.Precision.HIGHEST)
    c12_pair = jnp.dot(jnp.dot(type_hot_a, c12_sym, precision=lax.Precision.HIGHEST), type_hot_b.T, precision=lax.Precision.HIGHEST)
    charge_pair = pack_a[3][:, None] * pack_b[3][None, :]
    occupied_pair = pack_a[5][:, None] * pack_b[5][None, :] * pair_mask
    edge_inverse = 1.0 / (CUT_SQUARE + SOFTEN)
    edge_cube = edge_inverse ** 3

    def pair_energy(position_a, position_b):
        separation = position_b[:, None, :] - position_a[:, :, None] + offset[:, None, None]
        dist_square = lax.optimization_barrier(jnp.sum(separation * separation, axis=0))
        inverse = 1.0 / (dist_square + SOFTEN)
        inverse_cube = inverse * inverse * inverse
        coulomb = charge_pair * (jnp.sqrt(inverse) - edge_inverse ** 0.5)
        dispersion = c12_pair * (inverse_cube * inverse_cube - edge_cube * edge_cube) - c6_pair * (inverse_cube - edge_cube)
        cutoff_taper = jnp.maximum(1.0 - dist_square / CUT_SQUARE, 0.0)
        return ENERGY_UNIT * jnp.sum((coulomb + dispersion) * cutoff_taper * cutoff_taper * occupied_pair)
    energy, (grad_a, grad_b) = jax.value_and_grad(pair_energy, argnums=(0, 1))(pack_a[:3], pack_b[:3])
    return (energy, -grad_a, -grad_b)

def cell_batch(packs_a, packs_b, c6_sym, c12_sym, offset, pair_mask):

    def single(tiles):
        return tile_terms(tiles[0], tiles[1], c6_sym, c12_sym, offset, pair_mask)
    return lax.map(single, (packs_a, packs_b), batch_size=8)

def reference(coords, charges, atom_types, counts, c6_table, c12_table):
    c6_sym = 0.5 * (c6_table + c6_table.T)
    c12_sym = 0.5 * (c12_table + c12_table.T)
    packed = pack_cells(coords, charges, atom_types, counts)
    grid_shape = packed.shape[:3]
    slot_count = packed.shape[-1]
    upper_pairs = jnp.triu(jnp.ones((slot_count, slot_count), jnp.float32), 1)
    all_pairs = jnp.ones((slot_count, slot_count), jnp.float32)
    forces = jnp.zeros(grid_shape + (3, slot_count), jnp.float32)
    energy_sum = jnp.zeros((), jnp.float32)
    for source, target in ((0, 0),) + CELL_PAIRS:
        corner_a = corner_bits(source)
        corner_b = corner_bits(target)
        cells_a = jnp.roll(packed, (-corner_a[0], -corner_a[1], -corner_a[2]), axis=(0, 1, 2))
        cells_b = jnp.roll(packed, (-corner_b[0], -corner_b[1], -corner_b[2]), axis=(0, 1, 2))
        offset = jnp.array([(corner_b[k] - corner_a[k]) * CELL_EDGE for k in range(3)], jnp.float32)
        pair_mask = upper_pairs if source == target else all_pairs
        energies, force_a, force_b = cell_batch(cells_a.reshape((-1, 6, slot_count)), cells_b.reshape((-1, 6, slot_count)), c6_sym, c12_sym, offset, pair_mask)
        force_a = jnp.roll(force_a.reshape(grid_shape + (3, slot_count)), corner_a, axis=(0, 1, 2))
        force_b = jnp.roll(force_b.reshape(grid_shape + (3, slot_count)), corner_b, axis=(0, 1, 2))
        forces = forces + force_a + force_b
        energy_sum = energy_sum + jnp.sum(energies)
    return (forces, energy_sum.reshape(1))
```

```python
import functools

import jax
import jax.numpy as jnp
from jax import lax
from jax.experimental import pallas as pl
from jax.experimental.pallas import tpu as pltpu
from jax.sharding import PartitionSpec as P

CELL_EDGE = 1.1
SOFTEN = 0.09
ENERGY_UNIT = 0.1
EDGE_V = 1.0 / (1.0 + SOFTEN)
E0 = EDGE_V**0.5
E3 = EDGE_V**3
E6 = E3 * E3
STRIP = 16
OFFSETS = (
    (0, 0, 1), (0, 1, -1), (0, 1, 0), (0, 1, 1),
    (1, -1, -1), (1, -1, 0), (1, -1, 1),
    (1, 0, -1), (1, 0, 0), (1, 0, 1),
    (1, 1, -1), (1, 1, 0), (1, 1, 1), (0, 0, 0),
)
AXIS_SHIFTS = ((0, 0), (0, 1), (1, -1), (1, 0), (1, 1), (2, -1), (2, 0), (2, 1))
FEATS = 32


def shifted(block, axis, distance):
    n = lax.axis_size(axis)
    route = [((i - distance) % n, i) for i in range(n)]
    return lax.ppermute(block, axis, route)


def from_both(first, last, axis):
    if lax.axis_size(axis) == 2:
        both = shifted(jnp.stack([first, last]), axis, 1)
        return both[0], both[1]
    return shifted(first, axis, -1), shifted(last, axis, 1)


def ring_sum(value, axis):
    total = value
    for distance in range(1, lax.axis_size(axis)):
        total = total + shifted(value, axis, distance)
    return total


def returned(first, last, energy, axis):
    if lax.axis_size(axis) != 2:
        return (*from_both(first, last, axis), ring_sum(energy, axis))
    slots = energy.shape[-1]
    rows = jnp.stack([first, last]).reshape(-1, slots)
    got = shifted(jnp.concatenate([rows, energy]), axis, 1)
    both = got[:-1].reshape(2, *first.shape)
    return both[0], both[1], energy + got[-1:]


def rounded(value):
    return value.astype(jnp.bfloat16).astype(jnp.float32)


def two_parts(value):
    high = rounded(value)
    return high, rounded(value - high)


def three_parts(value):
    high = rounded(value)
    rest = value - high
    middle = rounded(rest)
    return high, middle, rounded(rest - middle)


def pick_rows(rows, choices):
    out = jnp.zeros(rows.shape, jnp.float32)
    for r, value in enumerate(choices):
        if value is not None:
            out = jnp.where(rows == r, value, out)
    return out


def dot(a, b):
    return jnp.dot(a, b, preferred_element_type=jnp.float32)


def pair_kernel(cx, cy, cz, nt, ext_ref, c6_ref, c12_ref, force_ref, energy_ref,
                lh, lx, qb, pos, wc, wk, blocks, qrow, xi, d1, d2, gg, fb, fa):
    ey = cy + 2
    ez = cz + 2
    slots = 128
    n_ext = (cx + 1) * ey * ez
    bf = jnp.bfloat16
    rows = lax.broadcasted_iota(jnp.int32, (8, slots), 0)
    ids = lax.broadcasted_iota(jnp.int32, (nt, slots), 0).astype(jnp.float32)
    c6 = c6_ref[...]
    c12 = c12_ref[...]
    c6 = (0.5 * ENERGY_UNIT) * (c6 + c6.T)
    c12 = (0.5 * ENERGY_UNIT) * (c12 + c12.T)
    both = jnp.concatenate([c12, c6], axis=0)
    high = both.astype(bf)
    low = (both - high.astype(jnp.float32)).astype(bf)
    const = (E3 * c6 - E6 * c12).astype(bf)
    zero_feats = jnp.zeros((nt - FEATS, slots), jnp.float32)

    def positions(f):
        parts = []
        for k in range(3):
            parts.append(two_parts(f[k : k + 1, :] - 0.5 * CELL_EDGE))
        return parts

    def prepare(c, carry):
        f = ext_ref[c]
        hot = (ids == f[4:5, :]).astype(jnp.float32)
        parts = positions(f)
        one = jnp.ones((1, slots), jnp.float32)
        feats = []
        norm = None
        for h, m in parts:
            feats.append(pick_rows(rows, (h, h, m, m, one, one, one)))
            x = h + m
            norm = x * x if norm is None else norm + x * x
        qh, qm = two_parts(f[3:4, :])
        feats.append(pick_rows(rows, (*three_parts(norm), qh, qh, qm, qm)))
        (xh, xm), (yh, ym), (zh, zm) = parts
        pos[c] = pick_rows(rows, (xh, xm, yh, ym, zh, zm, one))
        full = jnp.concatenate([hot, *feats, zero_feats], axis=0).astype(bf)
        lx[c] = full.T
        hot = hot.astype(bf)
        lh[c] = jnp.concatenate([hot, hot], axis=0).T
        qb[c] = jnp.broadcast_to(f[3:4, :], (slots, slots)).T
        return carry

    lax.fori_loop(0, n_ext, prepare, 0)

    def ext_of(a):
        x = a // (cy * cz)
        y = (a // cz) % cy
        z = a % cz
        return (x * ey + y + 1) * ez + z + 1

    def weights(a, carry):
        f = ext_ref[ext_of(a)]
        hot = (ids == f[4:5, :]).astype(jnp.float32).astype(bf)
        th = dot(high, hot).astype(bf)
        tl = dot(low, hot).astype(bf)
        wc[a, :, :slots] = jnp.concatenate([th[:nt], tl[:nt]], axis=0)
        wc[a, :, slots:] = jnp.concatenate([th[nt:], tl[nt:]], axis=0)
        kk = dot(const, hot)
        q = f[3:4, :]
        qh, qm = two_parts((-ENERGY_UNIT * E0) * q)
        qblock = pick_rows(rows, (None, None, None, qh, qm, qh, qm))
        zero = jnp.zeros((8, slots), jnp.float32)
        wk[a] = jnp.concatenate([kk, zero, zero, zero, qblock, zero_feats], axis=0).astype(bf)
        for n, (k, shift) in enumerate(AXIS_SHIFTS):
            h, m = two_parts(f[k : k + 1, :] - (0.5 * CELL_EDGE + shift * CELL_EDGE))
            y = h + m
            sq = y * y
            if k == 0:
                sq = sq + SOFTEN
            h2 = -2.0 * h
            m2 = -2.0 * m
            blocks[a, n] = pick_rows(rows, (h2, m2, h2, m2, *three_parts(sq)))
        qrow[a] = jnp.broadcast_to(ENERGY_UNIT * q, (8, slots))
        group = pos[ext_of(a)]
        xt = jnp.concatenate([group] * (slots // 8), axis=0).T.astype(bf)
        xi[a] = jnp.concatenate([xt, xt], axis=0)
        return carry

    lax.fori_loop(0, cx * cy * cz, weights, 0)

    norm_block = jnp.where(rows < 3, 1.0, 0.0)
    zero_hot = jnp.zeros((nt, slots), bf)
    zero_tail = zero_feats.astype(bf)
    strip_rows = lax.broadcasted_iota(jnp.int32, (STRIP, slots), 0)
    strip_lanes = lax.broadcasted_iota(jnp.int32, (STRIP, slots), 1)

    def neighbour(a, o):
        return ext_of(a) + (o[0] * ey + o[1]) * ez + o[2]

    def forward(a, n):
        o = OFFSETS[n]
        b = neighbour(a, o)
        d1[n % 2] = dot(lh[b], wc[a])
        picks = [AXIS_SHIFTS.index((k, o[k])) for k in range(3)]
        near = jnp.concatenate([blocks[a, p] for p in picks] + [norm_block], axis=0).astype(bf)
        w = jnp.concatenate([zero_hot, near, zero_tail], axis=0)
        d2[n % 2] = dot(lx[b], jnp.concatenate([w, wk[a]], axis=1))

    def compute(a, n, e_acc):
        o = OFFSETS[n]
        b = neighbour(a, o)
        q = qrow[a]
        q = jnp.concatenate([q, q], axis=0)
        own = o == (0, 0, 0)
        for r in range(0, slots, STRIP):
            at = pl.ds(r, STRIP)
            t = d2[n % 2, at, :slots]
            kk = d2[n % 2, at, slots:]
            c12 = d1[n % 2, at, :slots]
            c6 = d1[n % 2, at, slots:]
            charge = qb[b, at, :] * q
            s = lax.rsqrt(t)
            v = s * s
            z3 = v * v * v
            w = jnp.maximum((1.0 + SOFTEN) - t, 0.0)
            if own:
                w = jnp.where(strip_rows + r == strip_lanes, 0.0, w)
            p = charge * s
            m = c12 * z3
            a1 = m - c6
            u = z3 * a1 + p + kk
            h = (z3 * (a1 + m)) * 6.0 + p
            uw = u * w
            e = uw * w
            e_acc = e_acc + (0.5 * e if own else e)
            g = w * (v * w * h) + 4.0 * uw
            gh = g.astype(bf)
            gg[n % 2, at, :slots] = gh
            gg[n % 2, at, slots:] = (g - gh.astype(jnp.float32)).astype(bf)
        return e_acc

    def spread(a, n):
        o = OFFSETS[n]
        b = neighbour(a, o)
        g = gg[n % 2]
        if o != (0, 0, 0):
            out = dot(g, xi[a])
            fb[b, :, 8 * n : 8 * n + 8] = out[:, 8 * n : 8 * n + 8]
        left = pos[b].astype(bf)
        got = dot(left, g)
        fa[n] = got[:, :slots] + got[:, slots:]

    def clear(c, carry):
        fb[c] = jnp.zeros((slots, slots), jnp.float32)
        return carry

    lax.fori_loop(0, n_ext, clear, 0)
    count = len(OFFSETS)

    def shift_sum(parts):
        total = None
        extra = [None, None, None]
        for n, part in parts:
            total = part if total is None else total + part
            for k in range(3):
                s = OFFSETS[n][k]
                if s:
                    term = part if s > 0 else -part
                    extra[k] = term if extra[k] is None else extra[k] + term
        return total, extra

    def cell(a, e_acc):
        forward(a, 0)
        for n in range(count):
            if n + 1 < count:
                forward(a, n + 1)
            e_acc = compute(a, n, e_acc)
            if n:
                spread(a, n - 1)
        spread(a, count - 1)
        total, extra = shift_sum([(n, fa[n]) for n in range(count)])
        x = pos[ext_of(a)]
        s = total[6:7]
        for k in range(3):
            here = x[2 * k : 2 * k + 1] + x[2 * k + 1 : 2 * k + 2]
            moved = total[2 * k : 2 * k + 1] + total[2 * k + 1 : 2 * k + 2] + CELL_EDGE * extra[k][6:7]
            force_ref[ext_of(a), k : k + 1, :] = here * s - moved
        return e_acc

    force_ref[...] = jnp.zeros_like(force_ref)
    e = lax.fori_loop(0, cx * cy * cz, cell, jnp.zeros((STRIP, slots), jnp.float32))
    energy_ref[...] = e[:8] + e[8:]

    def gather(c, carry):
        turned = fb[c].T
        total, extra = shift_sum([(n, turned[8 * n : 8 * n + 8]) for n in range(count - 1)])
        x = pos[c]
        s = total[6:7]
        for k in range(3):
            here = x[2 * k : 2 * k + 1] + x[2 * k + 1 : 2 * k + 2]
            moved = total[2 * k : 2 * k + 1] + total[2 * k + 1 : 2 * k + 2] - CELL_EDGE * extra[k][6:7]
            force_ref[c, k : k + 1, :] += here * s - moved
        return carry

    lax.fori_loop(0, n_ext, gather, 0)


def pair_call(cx, cy, cz, nt, slots, ext, c6_table, c12_table):
    n_ext = (cx + 1) * (cy + 2) * (cz + 2)
    n = cx * cy * cz
    vm = pl.BlockSpec(memory_space=pltpu.VMEM)
    bf = jnp.bfloat16
    return pl.pallas_call(
        functools.partial(pair_kernel, cx, cy, cz, nt),
        out_shape=(
            jax.ShapeDtypeStruct((n_ext, 3, slots), jnp.float32),
            jax.ShapeDtypeStruct((8, slots), jnp.float32),
        ),
        in_specs=[vm, vm, vm],
        out_specs=(vm, vm),
        scratch_shapes=[
            pltpu.VMEM((n_ext, slots, slots), bf),
            pltpu.VMEM((n_ext, slots, slots), bf),
            pltpu.VMEM((n_ext, slots, slots), jnp.float32),
            pltpu.VMEM((n_ext, 8, slots), jnp.float32),
            pltpu.VMEM((n, slots, 2 * slots), bf),
            pltpu.VMEM((n, slots, slots), bf),
            pltpu.VMEM((n, 8, 8, slots), jnp.float32),
            pltpu.VMEM((n, 8, slots), jnp.float32),
            pltpu.VMEM((n, 2 * slots, slots), bf),
            pltpu.VMEM((2, slots, 2 * slots), jnp.float32),
            pltpu.VMEM((2, slots, 2 * slots), jnp.float32),
            pltpu.VMEM((2, slots, 2 * slots), bf),
            pltpu.VMEM((n_ext, slots, slots), jnp.float32),
            pltpu.VMEM((len(OFFSETS), 8, slots), jnp.float32),
        ],
        compiler_params=pltpu.CompilerParams(vmem_limit_bytes=56 * 2**20),
    )(ext, c6_table, c12_table)


def on_device(coords, charges, atom_types, counts, c6_table, c12_table):
    cx, cy, cz, _, slots = coords.shape
    nt = c6_table.shape[0]
    occ = jnp.arange(slots, dtype=jnp.int32) < counts[..., None]
    charge = jnp.where(occ, charges, 0.0)
    kind = jnp.where(occ, atom_types, nt).astype(jnp.float32)
    ext = jnp.concatenate(
        [coords, charge[..., None, :], kind[..., None, :], jnp.zeros((cx, cy, cz, 3, slots), jnp.float32)], axis=3
    )
    up = shifted(ext[:1], "gx", -1)
    ext = jnp.concatenate([ext, up], axis=0)
    above, below = from_both(ext[:, :1], ext[:, -1:], "gy")
    ext = jnp.concatenate([below, ext, above], axis=1)
    above, below = from_both(ext[:, :, :1], ext[:, :, -1:], "gz")
    ext = jnp.concatenate([below, ext, above], axis=2)
    ex, ey, ez = cx + 1, cy + 2, cz + 2
    forces, energy = pair_call(cx, cy, cz, nt, slots, ext.reshape(ex * ey * ez, 8, slots), c6_table, c12_table)
    energy = jnp.sum(energy, axis=0, keepdims=True)
    forces = forces.reshape(ex, ey, ez, 3, slots)
    low, high = from_both(forces[:, :, :1], forces[:, :, -1:], "gz")
    energy = ring_sum(energy, "gx")
    forces = forces[:, :, 1:-1].at[:, :, -1:].add(low).at[:, :, :1].add(high)
    low, high, energy = returned(forces[:, :1], forces[:, -1:], energy, "gy")
    forces = forces[:, 1:-1].at[:, -1:].add(low).at[:, :1].add(high)
    back = shifted(forces[cx:], "gx", 1)
    forces = forces[:cx].at[:1].add(back)
    energy = jnp.sum(ring_sum(energy, "gz"))
    return forces, energy.reshape(1)


def solution(mesh):
    return jax.shard_map(
        on_device,
        mesh=mesh,
        in_specs=(
            P(("groups", "gx"), "gy", "gz", None, None),
            P(("groups", "gx"), "gy", "gz", None),
            P(("groups", "gx"), "gy", "gz", None),
            P(("groups", "gx"), "gy", "gz"),
            P(),
            P(),
        ),
        out_specs=(P(("groups", "gx"), "gy", "gz", None, None), P("groups")),
        check_vma=False,
    )
```

```python
import functools

import jax
import jax.numpy as jnp
from jax import lax
from jax.experimental import pallas as pl
from jax.experimental.pallas import tpu as pltpu
from jax.sharding import PartitionSpec as P

CELL_EDGE = 1.1
SOFTEN = 0.09
ENERGY_UNIT = 0.1
EDGE_V = 1.0 / (1.0 + SOFTEN)
E0 = EDGE_V**0.5
E3 = EDGE_V**3
STRIP = 16
GROUP = 2
OFFSETS = (
    (0, 0, 1), (0, 1, -1), (0, 1, 0), (0, 1, 1),
    (1, -1, -1), (1, -1, 0), (1, -1, 1),
    (1, 0, -1), (1, 0, 0), (1, 0, 1),
    (1, 1, -1), (1, 1, 0), (1, 1, 1), (0, 0, 0),
)
AXIS_SHIFTS = ((0, 0), (0, 1), (1, -1), (1, 0), (1, 1), (2, -1), (2, 0), (2, 1))
FEATS = 32


def rounded(value):
    return value.astype(jnp.bfloat16).astype(jnp.float32)


def two_parts(value):
    high = rounded(value)
    return high, rounded(value - high)


def three_parts(value):
    high = rounded(value)
    rest = value - high
    middle = rounded(rest)
    return high, middle, rounded(rest - middle)


def pick_rows(rows, choices):
    out = jnp.zeros(rows.shape, jnp.float32)
    for r, value in enumerate(choices):
        if value is not None:
            out = jnp.where(rows == r, value, out)
    return out


def dot(a, b):
    return jnp.dot(a, b, preferred_element_type=jnp.float32)


def unroll_of(count, most):
    return max(u for u in range(1, most + 1) if count % u == 0)


def unrolled(count, most, body):
    u = unroll_of(count, most)

    def step(i, carry):
        for k in range(u):
            body(i * u + k)
        return carry

    lax.fori_loop(0, count // u, step, 0)


def pair_kernel(cx, cy, cz, nt, ext_ref, c6_ref, c12_ref, force_ref, energy_ref,
                lh, lc, pos, wc, blocks, xi, gg, fb, fa):
    ey = cy + 2
    ez = cz + 2
    slots = 128
    n_ext = (cx + 1) * ey * ez
    n_own = cx * cy * cz
    bf = jnp.bfloat16
    rows = lax.broadcasted_iota(jnp.int32, (8, slots), 0)
    ids = lax.broadcasted_iota(jnp.int32, (nt, slots), 0).astype(jnp.float32)
    c6 = c6_ref[...]
    c12 = c12_ref[...]
    c12 = (0.5 * ENERGY_UNIT) * (c12 + c12.T)
    c6 = (0.5 * ENERGY_UNIT) * (c6 + c6.T) - (2.0 * E3) * c12
    both = jnp.concatenate([c12, c6], axis=0)
    high = both.astype(bf)
    low = (both - high.astype(jnp.float32)).astype(bf)
    one = jnp.ones((1, slots), jnp.float32)

    def prepare(c):
        f = ext_ref[c]
        hot = (ids == f[4:5, :]).astype(jnp.float32).astype(bf)
        parts = [two_parts(f[k : k + 1, :] - 0.5 * CELL_EDGE) for k in range(3)]
        feats = []
        norm = None
        for h, m in parts:
            feats.append(pick_rows(rows, (h, h, m, m, one, one, one)))
            x = h + m
            norm = x * x if norm is None else norm + x * x
        qh, qm = two_parts(f[3:4, :])
        feats.append(pick_rows(rows, (*three_parts(norm), qh, qh, qm, qm)))
        (xh, xm), (yh, ym), (zh, zm) = parts
        pos[c] = pick_rows(rows, (xh, xm, yh, ym, zh, zm, one))
        lc[c] = jnp.concatenate(feats, axis=0).astype(bf).T
        lh[c] = jnp.concatenate([hot, hot], axis=0).T

    unrolled(n_ext, 5, prepare)

    def ext_of(a):
        x = a // (cy * cz)
        y = (a // cz) % cy
        z = a % cz
        return (x * ey + y + 1) * ez + z + 1

    def weights(a):
        f = ext_ref[ext_of(a)]
        hot = (ids == f[4:5, :]).astype(jnp.float32).astype(bf)
        th = dot(high, hot).astype(bf)
        tl = dot(low, hot).astype(bf)
        wc[a, :, :slots] = jnp.concatenate([th[:nt], tl[:nt]], axis=0)
        wc[a, :, slots:] = jnp.concatenate([th[nt:], tl[nt:]], axis=0)
        for n, (k, shift) in enumerate(AXIS_SHIFTS):
            h, m = two_parts(f[k : k + 1, :] - (0.5 * CELL_EDGE + shift * CELL_EDGE))
            y = h + m
            sq = y * y
            if k == 0:
                sq = sq + SOFTEN
            h2 = -2.0 * h
            m2 = -2.0 * m
            blocks[a, n] = pick_rows(rows, (h2, m2, h2, m2, *three_parts(sq)))
        qh, qm = two_parts(ENERGY_UNIT * f[3:4, :])
        blocks[a, len(AXIS_SHIFTS)] = pick_rows(rows, (None, None, None, qh, qm, qh, qm))
        group = pos[ext_of(a)]
        xt = jnp.concatenate([group] * (slots // 8), axis=0).astype(bf).T
        xi[a] = jnp.concatenate([xt, xt], axis=0)

    unrolled(n_own, 4, weights)

    norm_block = jnp.where(rows < 3, 1.0, 0.0)
    zero_block = jnp.zeros((8, slots), jnp.float32)
    strip_rows = lax.broadcasted_iota(jnp.int32, (STRIP, slots), 0)
    strip_lanes = lax.broadcasted_iota(jnp.int32, (STRIP, slots), 1)
    count = len(OFFSETS)
    items = count // GROUP

    def neighbour(a, n):
        o = OFFSETS[n]
        return ext_of(a) + (o[0] * ey + o[1]) * ez + o[2]

    def forward(a, i):
        members = range(i * GROUP, (i + 1) * GROUP)
        v1 = dot(jnp.concatenate([lh[neighbour(a, n)] for n in members], axis=0), wc[a])
        v2 = []
        charge = jnp.concatenate([zero_block] * 3 + [blocks[a, len(AXIS_SHIFTS)]], axis=0).astype(bf)
        for j, n in enumerate(members):
            picks = [AXIS_SHIFTS.index((k, OFFSETS[n][k])) for k in range(3)]
            near = jnp.concatenate([blocks[a, p] for p in picks] + [norm_block], axis=0).astype(bf)
            v2.append(dot(lc[neighbour(a, n)], jnp.concatenate([near, charge], axis=1)))
        return v1, v2

    def compute(i, e_acc, vals):
        v1, v2 = vals

        for j in range(GROUP):
            own = OFFSETS[i * GROUP + j] == (0, 0, 0)
            for r in range(0, slots, STRIP):
                at = pl.ds(j * slots + r, STRIP)
                t = v2[j][r:r+STRIP, :slots]
                charge = v2[j][r:r+STRIP, slots:]
                c12 = v1[j*slots+r:j*slots+r+STRIP, :slots]
                c6 = v1[j*slots+r:j*slots+r+STRIP, slots:]
                s = lax.rsqrt(t)
                v = s * s
                z3 = v * v * v
                w = jnp.maximum((1.0 + SOFTEN) - t, 0.0)
                if own:
                    w = jnp.where(strip_rows + r == strip_lanes, 0.0, w)
                y = z3 - E3
                m = c12 * y
                b1 = m - c6
                p = charge * s
                u = y * b1 + charge * (s - E0)
                h = (z3 * (b1 + m)) * 6.0 + p
                uw = u * w
                e = uw * w
                e_acc = e_acc + (0.5 * e if own else e)
                g = w * (v * w * h) + 4.0 * uw
                gh = g.astype(bf)
                gg[i, at, :slots] = gh
                gg[i, at, slots:] = (g - gh.astype(jnp.float32)).astype(bf)
        return e_acc

    def spread(a, i):
        out = dot(gg[i], xi[a])
        for j in range(GROUP):
            n = i * GROUP + j
            b = neighbour(a, n)
            if OFFSETS[n] != (0, 0, 0):
                fb[b, :, 8 * n : 8 * n + 8] = out[j * slots : (j + 1) * slots, 8 * n : 8 * n + 8]
            got = dot(pos[b].astype(bf), gg[i, pl.ds(j * slots, slots), :])
            fa[n] = got[:, :slots] + got[:, slots:]

    def clear(c):
        fb[c] = jnp.zeros((slots, slots), jnp.float32)

    unrolled(n_ext, 2, clear)

    def shift_sum(parts):
        total = None
        extra = [None, None, None]
        for n, part in parts:
            total = part if total is None else total + part
            for k in range(3):
                s = OFFSETS[n][k]
                if s:
                    term = part if s > 0 else -part
                    extra[k] = term if extra[k] is None else extra[k] + term
        return total, extra

    def finish(a):
        total, extra = shift_sum([(n, fa[n]) for n in range(count)])
        x = pos[ext_of(a)]
        s = total[6:7]
        for k in range(3):
            here = x[2 * k : 2 * k + 1] + x[2 * k + 1 : 2 * k + 2]
            moved = total[2 * k : 2 * k + 1] + total[2 * k + 1 : 2 * k + 2] + CELL_EDGE * extra[k][6:7]
            force_ref[ext_of(a), k : k + 1, :] = here * s - moved

    def cell(a, e_acc):
        before = jnp.maximum(a - 1, 0)
        after = jnp.minimum(a + 1, n_own - 1)
        vals = forward(a, 0)
        for i in range(items):
            nxt = forward(a, i + 1) if i + 1 < items else None
            e_acc = compute(i, e_acc, vals)
            vals = nxt
            if i:
                spread(a, i - 1)
            else:
                spread(before, items - 1)
                finish(before)
        return e_acc

    force_ref[...] = jnp.zeros_like(force_ref)
    gg[items - 1] = jnp.zeros_like(gg[items - 1])
    fa[...] = jnp.zeros_like(fa)
    e = lax.fori_loop(0, n_own, cell, jnp.zeros((STRIP, slots), jnp.float32))
    spread(n_own - 1, items - 1)
    finish(n_own - 1)
    energy_ref[...] = e[:8] + e[8:]

    def gather(c):
        turned = fb[c].T
        total, extra = shift_sum([(n, turned[8 * n : 8 * n + 8]) for n in range(count - 1)])
        x = pos[c]
        s = total[6:7]
        for k in range(3):
            here = x[2 * k : 2 * k + 1] + x[2 * k + 1 : 2 * k + 2]
            moved = total[2 * k : 2 * k + 1] + total[2 * k + 1 : 2 * k + 2] - CELL_EDGE * extra[k][6:7]
            force_ref[c, k : k + 1, :] += here * s - moved

    unrolled(n_ext, 5, gather)


def pair_call(cx, cy, cz, nt, slots, ext, c6_table, c12_table):
    n_ext = (cx + 1) * (cy + 2) * (cz + 2)
    n = cx * cy * cz
    vm = pl.BlockSpec(memory_space=pltpu.VMEM)
    bf = jnp.bfloat16
    items = len(OFFSETS) // GROUP
    return pl.pallas_call(
        functools.partial(pair_kernel, cx, cy, cz, nt),
        out_shape=(
            jax.ShapeDtypeStruct((n_ext, 3, slots), jnp.float32),
            jax.ShapeDtypeStruct((8, slots), jnp.float32),
        ),
        in_specs=[vm, vm, vm],
        out_specs=(vm, vm),
        scratch_shapes=[
            pltpu.VMEM((n_ext, slots, slots), bf),
            pltpu.VMEM((n_ext, slots, FEATS), bf),
            pltpu.VMEM((n_ext, 8, slots), jnp.float32),
            pltpu.VMEM((n, slots, 2 * slots), bf),
            pltpu.VMEM((n, len(AXIS_SHIFTS) + 1, 8, slots), jnp.float32),
            pltpu.VMEM((n, 2 * slots, slots), bf),
            pltpu.VMEM((items, GROUP * slots, 2 * slots), bf),
            pltpu.VMEM((n_ext, slots, slots), jnp.float32),
            pltpu.VMEM((len(OFFSETS), 8, slots), jnp.float32),
        ],
        compiler_params=pltpu.CompilerParams(vmem_limit_bytes=56 * 2**20),
    )(ext, c6_table, c12_table)


MESH = pl.DeviceIdType.MESH
AXES = ("gx", "gy", "gz")
REGIONS = (
    (1, 0, 0), (1, 1, 0), (1, -1, 0), (1, 0, 1), (1, 0, -1), (1, 1, 1), (1, 1, -1), (1, -1, 1), (1, -1, -1),
    (0, 1, 0), (0, 1, 1), (0, 1, -1), (0, 0, 1), (0, 0, -1),
)


def sizes():
    return tuple(lax.axis_size(name) for name in AXES)


def device_at(step):
    return {name: lax.rem(lax.axis_index(name) + d % n, n) for name, d, n in zip(AXES, step, sizes())}


def wrapped(step):
    return tuple(d % n for d, n in zip(step, sizes()))


def meet(steps):
    barrier = pltpu.get_barrier_semaphore()
    near = {wrapped(s) for s in steps} | {wrapped([-d for d in s]) for s in steps}
    near = sorted(near - {(0, 0, 0)})
    for step in near:
        pl.semaphore_signal(barrier, inc=1, device_id=device_at(step), device_id_type=MESH)
    pl.semaphore_wait(barrier, len(near))


def halo_at(region, size):
    cx, cy, cz = size
    x = pl.ds(cx, 1) if region[0] else pl.ds(0, cx)
    y = {-1: pl.ds(0, 1), 0: pl.ds(1, cy), 1: pl.ds(cy + 1, 1)}[region[1]]
    z = {-1: pl.ds(0, 1), 0: pl.ds(1, cz), 1: pl.ds(cz + 1, 1)}[region[2]]
    return x, y, z


def edge_at(region, size):
    cx, cy, cz = size
    x = pl.ds(0, 1) if region[0] else pl.ds(0, cx)
    y = {-1: pl.ds(cy - 1, 1), 0: pl.ds(0, cy), 1: pl.ds(0, 1)}[region[1]]
    z = {-1: pl.ds(cz - 1, 1), 0: pl.ds(0, cz), 1: pl.ds(0, 1)}[region[2]]
    return x, y, z


def halo_kernel(size, local_ref, ext_ref, send_sem, recv_sem):
    cx, cy, cz = size
    ext_ref[pl.ds(0, cx), pl.ds(1, cy), pl.ds(1, cz)] = local_ref[...]
    ext_ref[0, 0] = jnp.zeros_like(ext_ref[0, 0])
    meet(REGIONS)
    copies = []
    for n, region in enumerate(REGIONS):
        copy = pltpu.make_async_remote_copy(
            src_ref=local_ref.at[edge_at(region, size)],
            dst_ref=ext_ref.at[halo_at(region, size)],
            send_sem=send_sem.at[n],
            recv_sem=recv_sem.at[n],
            device_id=device_at([-d for d in region]),
            device_id_type=MESH,
        )
        copy.start()
        copies.append(copy)
    for copy in copies:
        copy.wait()


def halo_call(local):
    cx, cy, cz, rows, slots = local.shape
    vm = pl.BlockSpec(memory_space=pltpu.VMEM)
    return pl.pallas_call(
        functools.partial(halo_kernel, (cx, cy, cz)),
        out_shape=jax.ShapeDtypeStruct((cx + 1, cy + 2, cz + 2, rows, slots), jnp.float32),
        in_specs=[vm],
        out_specs=vm,
        scratch_shapes=[pltpu.SemaphoreType.DMA((len(REGIONS),))] * 2,
        compiler_params=pltpu.CompilerParams(collective_id=0, has_side_effects=True),
    )(local)


def phases():
    nx, ny, nz = sizes()
    plane = [(0, y, z) for y in range(ny) for z in range(nz)]
    if nx * ny * nz <= 16:
        return ([(x, y, z) for x in range(nx) for _, y, z in plane][1:],)
    return plane[1:], [(x, 0, 0) for x in range(1, nx)]


def return_kernel(size, part_ref, energy_ref, force_ref, total_ref, *scratch):
    sums = phases()
    buffers = scratch[: len(REGIONS)]
    arrived = scratch[len(REGIONS) : len(REGIONS) + len(sums)]
    mine, send_sem, recv_sem = scratch[len(REGIONS) + len(sums) : len(REGIONS) + len(sums) + 3]
    sum_sems = scratch[len(REGIONS) + len(sums) + 3 :]
    meet([*REGIONS, *(step for steps in sums for step in steps)])
    pending = []
    energy = energy_ref[...]

    def send_energy(p, source):
        copies = []
        for n, step in enumerate(sums[p]):
            copy = pltpu.make_async_remote_copy(
                src_ref=source,
                dst_ref=arrived[p].at[n],
                send_sem=sum_sems[2 * p].at[n],
                recv_sem=sum_sems[2 * p + 1].at[n],
                device_id=device_at(step),
                device_id_type=MESH,
            )
            copy.start()
            copies.append(copy)
        return copies

    first = send_energy(0, energy_ref)
    for n, region in enumerate(REGIONS):
        copy = pltpu.make_async_remote_copy(
            src_ref=part_ref.at[halo_at(region, size)],
            dst_ref=buffers[n],
            send_sem=send_sem.at[n],
            recv_sem=recv_sem.at[n],
            device_id=device_at(region),
            device_id_type=MESH,
        )
        copy.start()
        pending.append(copy)
    for p in range(len(sums)):
        copies = first if p == 0 else send_energy(p, mine)
        for n, copy in enumerate(copies):
            copy.wait()
            energy = energy + arrived[p][n]
        if p + 1 < len(sums):
            mine[...] = energy
    total_ref[...] = jnp.sum(energy, axis=0, keepdims=True)
    cx, cy, cz = size
    force_ref[...] = part_ref[pl.ds(0, cx), pl.ds(1, cy), pl.ds(1, cz)]
    for n, region in enumerate(REGIONS):
        pending[n].wait()
        force_ref[edge_at(region, size)] += buffers[n][...]


def return_call(part, energy, size):
    slots = part.shape[-1]
    vm = pl.BlockSpec(memory_space=pltpu.VMEM)
    sums = phases()

    def extent(region):
        return tuple(s.size for s in edge_at(region, size)) + part.shape[3:]

    return pl.pallas_call(
        functools.partial(return_kernel, size),
        out_shape=(
            jax.ShapeDtypeStruct((*size, *part.shape[3:]), jnp.float32),
            jax.ShapeDtypeStruct((1, slots), jnp.float32),
        ),
        in_specs=[vm, vm],
        out_specs=(vm, vm),
        scratch_shapes=[
            *(pltpu.VMEM(extent(region), jnp.float32) for region in REGIONS),
            *(pltpu.VMEM((len(steps), *energy.shape), jnp.float32) for steps in sums),
            pltpu.VMEM(energy.shape, jnp.float32),
            *[pltpu.SemaphoreType.DMA((len(REGIONS),))] * 2,
            *(pltpu.SemaphoreType.DMA((len(steps),)) for steps in sums for _ in range(2)),
        ],
        compiler_params=pltpu.CompilerParams(collective_id=1, has_side_effects=True),
    )(part, energy)


def on_device(coords, charges, atom_types, counts, c6_table, c12_table):
    cx, cy, cz, _, slots = coords.shape
    nt = c6_table.shape[0]
    occ = jnp.arange(slots, dtype=jnp.int32) < counts[..., None]
    charge = jnp.where(occ, charges, 0.0)
    kind = jnp.where(occ, atom_types, nt).astype(jnp.float32)
    local = jnp.concatenate(
        [coords, charge[..., None, :], kind[..., None, :], jnp.zeros((cx, cy, cz, 3, slots), jnp.float32)], axis=3
    )
    ext = halo_call(local)
    ex, ey, ez = cx + 1, cy + 2, cz + 2
    part, energy = pair_call(cx, cy, cz, nt, slots, ext.reshape(ex * ey * ez, 8, slots), c6_table, c12_table)
    forces, energy = return_call(part.reshape(ex, ey, ez, 3, slots), energy, (cx, cy, cz))
    return forces, jnp.sum(energy).reshape(1)


def solution(mesh):
    return jax.shard_map(
        on_device,
        mesh=mesh,
        in_specs=(
            P(("groups", "gx"), "gy", "gz", None, None),
            P(("groups", "gx"), "gy", "gz", None),
            P(("groups", "gx"), "gy", "gz", None),
            P(("groups", "gx"), "gy", "gz"),
            P(),
            P(),
        ),
        out_specs=(P(("groups", "gx"), "gy", "gz", None, None), P("groups")),
        check_vma=False,
    )
```

```python
import functools

import jax
import jax.numpy as jnp
from jax import lax
from jax.experimental import pallas as pl
from jax.experimental.pallas import tpu as pltpu
from jax.sharding import PartitionSpec as P

CELL_EDGE = 1.1
SOFTEN = 0.09
ENERGY_UNIT = 0.1
EDGE_V = 1.0 / (1.0 + SOFTEN)
E0 = EDGE_V**0.5
E3 = EDGE_V**3
STRIP = 128
WITHIN = ((0, 1, 2), (3, 13))
BEYOND = ((4, 5, 6), (7, 8, 9), (10, 11, 12))
OFFSETS = (
    (0, 0, 1), (0, 1, -1), (0, 1, 0), (0, 1, 1),
    (1, -1, -1), (1, -1, 0), (1, -1, 1),
    (1, 0, -1), (1, 0, 0), (1, 0, 1),
    (1, 1, -1), (1, 1, 0), (1, 1, 1), (0, 0, 0),
)
AXIS_SHIFTS = ((0, 0), (0, 1), (1, -1), (1, 0), (1, 1), (2, -1), (2, 0), (2, 1))
FEATS = 32


def rounded(value):
    return value.astype(jnp.bfloat16).astype(jnp.float32)


def two_parts(value):
    high = rounded(value)
    return high, rounded(value - high)


def three_parts(value):
    high = rounded(value)
    rest = value - high
    middle = rounded(rest)
    return high, middle, rounded(rest - middle)


def pick_rows(rows, choices):
    out = jnp.zeros(rows.shape, jnp.float32)
    for r, value in enumerate(choices):
        if value is not None:
            out = jnp.where(rows == r, value, out)
    return out


def dot(a, b):
    return jnp.dot(a, b, preferred_element_type=jnp.float32)


def unroll_of(count, most):
    return max(u for u in range(1, most + 1) if count % u == 0)


def unrolled(count, most, body):
    u = unroll_of(count, most)

    def step(i, carry):
        for k in range(u):
            body(i * u + k)
        return carry

    lax.fori_loop(0, count // u, step, 0)


MESH = pl.DeviceIdType.MESH
AXES = ("gx", "gy", "gz")
REGIONS = (
    (1, 0, 0), (1, 1, 0), (1, -1, 0), (1, 0, 1), (1, 0, -1), (1, 1, 1), (1, 1, -1), (1, -1, 1), (1, -1, -1),
    (0, 1, 0), (0, 1, 1), (0, 1, -1), (0, 0, 1), (0, 0, -1),
)


def sizes():
    return tuple(lax.axis_size(name) for name in AXES)


def device_at(step):
    return {name: lax.rem(lax.axis_index(name) + d % n, n) for name, d, n in zip(AXES, step, sizes())}


def wrapped(step):
    return tuple(d % n for d, n in zip(step, sizes()))


def meet(steps):
    barrier = pltpu.get_barrier_semaphore()
    near = {wrapped(s) for s in steps} | {wrapped([-d for d in s]) for s in steps}
    near = sorted(near - {(0, 0, 0)})
    for step in near:
        pl.semaphore_signal(barrier, inc=1, device_id=device_at(step), device_id_type=MESH)
    pl.semaphore_wait(barrier, len(near))


def halo_at(region, size):
    cx, cy, cz = size
    x = pl.ds(cx, 1) if region[0] else pl.ds(0, cx)
    y = {-1: pl.ds(0, 1), 0: pl.ds(1, cy), 1: pl.ds(cy + 1, 1)}[region[1]]
    z = {-1: pl.ds(0, 1), 0: pl.ds(1, cz), 1: pl.ds(cz + 1, 1)}[region[2]]
    return x, y, z


def edge_at(region, size):
    cx, cy, cz = size
    x = pl.ds(0, 1) if region[0] else pl.ds(0, cx)
    y = {-1: pl.ds(cy - 1, 1), 0: pl.ds(0, cy), 1: pl.ds(0, 1)}[region[1]]
    z = {-1: pl.ds(cz - 1, 1), 0: pl.ds(0, cz), 1: pl.ds(0, 1)}[region[2]]
    return x, y, z


def phases():
    nx, ny, nz = sizes()
    plane = [(0, y, z) for y in range(ny) for z in range(nz)]
    if nx * ny * nz <= 16:
        return ([(x, y, z) for x in range(nx) for _, y, z in plane][1:],)
    return plane[1:], [(x, 0, 0) for x in range(1, nx)]


def pair_kernel(size, nt, coords_ref, charge_ref, type_ref, count_ref, c6_ref, c12_ref, force_ref, energy_ref,
                local, ext, part, lh, lc, pos, wc, blocks, xi, gg, fb, fa, esum, *scratch):
    cx, cy, cz = size
    ey = cy + 2
    ez = cz + 2
    slots = 128
    n_ext = (cx + 1) * ey * ez
    n_own = cx * cy * cz
    bf = jnp.bfloat16
    buffers = scratch[: len(REGIONS)]
    send_sem, recv_sem, back_send, back_recv = scratch[len(REGIONS) : len(REGIONS) + 4]
    sums = phases()
    arrived = scratch[len(REGIONS) + 4 : len(REGIONS) + 4 + len(sums)]
    sum_sems = scratch[len(REGIONS) + 4 + len(sums) :]
    rows = lax.broadcasted_iota(jnp.int32, (8, slots), 0)
    lanes = lax.broadcasted_iota(jnp.int32, (1, slots), 1)
    ids = lax.broadcasted_iota(jnp.int32, (nt, slots), 0).astype(jnp.float32)
    one = jnp.ones((1, slots), jnp.float32)

    for x in range(cx):
        for y in range(cy):
            for z in range(cz):
                occupied = lanes < count_ref[x, y, z]
                charge = jnp.where(occupied, charge_ref[x, y, z : z + 1, :], 0.0)
                kind = jnp.where(occupied, type_ref[x, y, z : z + 1, :], nt).astype(jnp.float32)
                tile = jnp.concatenate([coords_ref[x, y, z], charge, kind, jnp.zeros((3, slots), jnp.float32)], axis=0)
                local[x, y, z] = tile
                ext[x, y + 1, z + 1] = tile

    meet([*REGIONS, *(step for steps in sums for step in steps)])
    copies = {}
    for n, region in enumerate(REGIONS):
        copies[region] = pltpu.make_async_remote_copy(
            src_ref=local.at[edge_at(region, size)],
            dst_ref=ext.at[halo_at(region, size)],
            send_sem=send_sem.at[n],
            recv_sem=recv_sem.at[n],
            device_id=device_at([-d for d in region]),
            device_id_type=MESH,
        )
    for plane in (0, 1):
        for region in REGIONS:
            if region[0] == plane:
                copies[region].start()

    c6 = c6_ref[...]
    c12 = c12_ref[...]
    c12 = (0.5 * ENERGY_UNIT) * (c12 + c12.T)
    c6 = (0.5 * ENERGY_UNIT) * (c6 + c6.T) - (2.0 * E3) * c12
    both = jnp.concatenate([c12, c6], axis=0)
    high = both.astype(bf)
    low = (both - high.astype(jnp.float32)).astype(bf)

    def flat(p):
        return (p[0] * ey + p[1]) * ez + p[2]

    def place(a):
        return a // (cy * cz), (a // cz) % cy + 1, a % cz + 1

    def prepare(p):
        c = flat(p)
        f = ext[p[0], p[1], p[2]]
        hot = (ids == f[4:5, :]).astype(jnp.float32).astype(bf)
        parts = [two_parts(f[k : k + 1, :] - 0.5 * CELL_EDGE) for k in range(3)]
        feats = []
        norm = None
        for h, m in parts:
            feats.append(pick_rows(rows, (h, h, m, m, one, one, one)))
            x = h + m
            norm = x * x if norm is None else norm + x * x
        qh, qm = two_parts(f[3:4, :])
        feats.append(pick_rows(rows, (*three_parts(norm), qh, qh, qm, qm)))
        (xh, xm), (yh, ym), (zh, zm) = parts
        pos[c] = pick_rows(rows, (xh, xm, yh, ym, zh, zm, one))
        lc[c] = jnp.concatenate(feats, axis=0).astype(bf).T
        lh[c] = jnp.concatenate([hot, hot], axis=0).T
        fb[c] = jnp.zeros((slots, slots), jnp.float32)

    def weights(a):
        x, y, z = place(a)
        f = ext[x, y, z]
        hot = (ids == f[4:5, :]).astype(jnp.float32).astype(bf)
        th = dot(high, hot).astype(bf)
        tl = dot(low, hot).astype(bf)
        wc[a, :, :slots] = jnp.concatenate([th[:nt], tl[:nt]], axis=0)
        wc[a, :, slots:] = jnp.concatenate([th[nt:], tl[nt:]], axis=0)
        for n, (k, shift) in enumerate(AXIS_SHIFTS):
            h, m = two_parts(f[k : k + 1, :] - (0.5 * CELL_EDGE + shift * CELL_EDGE))
            r = h + m
            sq = r * r
            if k == 0:
                sq = sq + SOFTEN
            h2 = -2.0 * h
            m2 = -2.0 * m
            blocks[a, n] = pick_rows(rows, (h2, m2, h2, m2, *three_parts(sq)))
        qh, qm = two_parts(ENERGY_UNIT * f[3:4, :])
        blocks[a, len(AXIS_SHIFTS)] = pick_rows(rows, (None, None, None, qh, qm, qh, qm))
        group = pos[flat((x, y, z))]
        xt = jnp.concatenate([group] * (slots // 8), axis=0).astype(bf).T
        xi[a] = jnp.concatenate([xt, xt], axis=0)

    norm_block = jnp.where(rows < 3, 1.0, 0.0)
    zero_block = jnp.zeros((8, slots), jnp.float32)
    strip_rows = lax.broadcasted_iota(jnp.int32, (STRIP, slots), 0)
    strip_lanes = lax.broadcasted_iota(jnp.int32, (STRIP, slots), 1)

    def neighbour(a, n):
        o = OFFSETS[n]
        return flat(place(a)) + (o[0] * ey + o[1]) * ez + o[2]

    def forward(a, members):
        v1 = dot(jnp.concatenate([lh[neighbour(a, n)] for n in members], axis=0), wc[a])
        v2 = []
        charge = jnp.concatenate([zero_block] * 3 + [blocks[a, len(AXIS_SHIFTS)]], axis=0).astype(bf)
        for n in members:
            picks = [AXIS_SHIFTS.index((k, OFFSETS[n][k])) for k in range(3)]
            near = jnp.concatenate([blocks[a, p] for p in picks] + [norm_block], axis=0).astype(bf)
            v2.append(dot(lc[neighbour(a, n)], jnp.concatenate([near, charge], axis=1)))
        return v1, v2

    def compute(i, members, e_acc, vals):
        v1, v2 = vals
        for j, n in enumerate(members):
            own = OFFSETS[n] == (0, 0, 0)
            for r in range(0, slots, STRIP):
                at = pl.ds(j * slots + r, STRIP)
                t = v2[j][r : r + STRIP, :slots]
                charge = v2[j][r : r + STRIP, slots:]
                c12p = v1[j * slots + r : j * slots + r + STRIP, :slots]
                c6p = v1[j * slots + r : j * slots + r + STRIP, slots:]
                s = lax.rsqrt(t)
                v = s * s
                z3 = v * v * v
                w = jnp.maximum((1.0 + SOFTEN) - t, 0.0)
                if own:
                    w = jnp.where(strip_rows + r == strip_lanes, 0.0, w)
                y = z3 - E3
                m = c12p * y
                b1 = m - c6p
                u = y * b1 + charge * (s - E0)
                h = (z3 * (b1 + m)) * 6.0 + charge * s
                uw = u * w
                e = jnp.sum((uw * w).reshape(STRIP // 8, 8, slots), axis=0)
                e_acc = e_acc + (0.5 * e if own else e)
                g = w * (v * w * h) + 4.0 * uw
                gh = g.astype(bf)
                gg[i, at, :slots] = gh
                gg[i, at, slots:] = (g - gh.astype(jnp.float32)).astype(bf)
        return e_acc

    def spread(a, i, members):
        out = dot(gg[i, pl.ds(0, slots * len(members)), :], xi[a])
        for j, n in enumerate(members):
            b = neighbour(a, n)
            if OFFSETS[n] != (0, 0, 0):
                fb[b, :, 8 * n : 8 * n + 8] = out[j * slots : (j + 1) * slots, 8 * n : 8 * n + 8]
            got = dot(pos[b].astype(bf), gg[i, pl.ds(j * slots, slots), :])
            fa[n] = got[:, :slots] + got[:, slots:]

    def shift_sum(parts):
        total = None
        extra = [zero_block] * 3
        for n, value in parts:
            total = value if total is None else total + value
            for k in range(3):
                o = OFFSETS[n][k]
                if o:
                    extra[k] = extra[k] + value if o > 0 else extra[k] - value
        return total, extra

    def force_of(c, parts, sign):
        total, extra = shift_sum(parts)
        x = pos[c]
        s = total[6:7]
        out = []
        for k in range(3):
            here = x[2 * k : 2 * k + 1] + x[2 * k + 1 : 2 * k + 2]
            moved = total[2 * k : 2 * k + 1] + total[2 * k + 1 : 2 * k + 2] + (sign * CELL_EDGE) * extra[k][6:7]
            out.append(here * s - moved)
        return jnp.concatenate(out, axis=0)

    def run(low_a, high_a, groups, e_acc):
        span = high_a - low_a
        names = [n for members in groups for n in members]
        last = len(groups) - 1
        gg[last] = jnp.zeros(gg.shape[1:], bf)
        fa[...] = jnp.zeros(fa.shape, jnp.float32)

        def finish(a):
            x, y, z = place(a)
            part[x, y, z] += force_of(flat((x, y, z)), [(n, fa[n]) for n in names], 1.0)

        def cell(a, e_acc):
            before = low_a + (a - low_a + span - 1) % span
            vals = forward(a, groups[0])
            for i, members in enumerate(groups):
                ahead = forward(a, groups[i + 1]) if i < last else None
                e_acc = compute(i, members, e_acc, vals)
                vals = ahead
                if i:
                    spread(a, i - 1, groups[i - 1])
                else:
                    spread(before, last, groups[last])
                    finish(before)
            return e_acc

        e_acc = lax.fori_loop(low_a, high_a, cell, e_acc)
        spread(high_a - 1, last, groups[last])
        finish(high_a - 1)
        return e_acc

    def gathered(c):
        turned = fb[c].T
        return force_of(c, [(n, turned[8 * n : 8 * n + 8]) for n in range(len(OFFSETS) - 1)], -1.0)

    def gather(p):
        part[p[0], p[1], p[2]] = gathered(flat(p))

    def top_row(body):
        unrolled(cx * ez, 5, lambda i: body((i // ez, cy + 1, i % ez)))

    def side_columns(body):
        unrolled(2 * cx * cy, 4, lambda i: body((i // (2 * cy), (i // 2) % cy + 1, (i % 2) * (cz + 1))))

    def far_plane(body):
        unrolled(ey * ez, 5, lambda i: body((cx, i // ez, i % ez)))

    def send_back(plane):
        for n, region in enumerate(REGIONS):
            if region[0] == plane:
                back[region] = pltpu.make_async_remote_copy(
                    src_ref=part.at[halo_at(region, size)],
                    dst_ref=buffers[n],
                    send_sem=back_send.at[n],
                    recv_sem=back_recv.at[n],
                    device_id=device_at(region),
                    device_id_type=MESH,
                )
                back[region].start()

    def send_energy(p):
        started = []
        for n, step in enumerate(sums[p]):
            copy = pltpu.make_async_remote_copy(
                src_ref=esum.at[p],
                dst_ref=arrived[p].at[n],
                send_sem=sum_sems[2 * p].at[n],
                recv_sem=sum_sems[2 * p + 1].at[n],
                device_id=device_at(step),
                device_id_type=MESH,
            )
            copy.start()
            started.append(copy)
        return started

    back = {}
    unrolled(n_own, 4, lambda a: prepare(place(a)))
    unrolled(n_own, 4, weights)
    part[...] = jnp.zeros(part.shape, jnp.float32)
    for region in REGIONS:
        if region[0] == 0:
            copies[region].wait()
    top_row(prepare)
    side_columns(prepare)
    half = n_own // 2
    e = run(0, half, WITHIN, zero_block)
    for region in REGIONS:
        if region[0] == 1:
            copies[region].wait()
    far_plane(prepare)
    e = run(0, n_own, BEYOND, e)
    far_plane(gather)
    send_back(1)
    e = run(half, n_own, WITHIN, e)
    esum[0] = e
    top_row(gather)
    side_columns(gather)
    started = send_energy(0)
    send_back(0)

    def own_force(a):
        x, y, z = place(a)
        force_ref[x, y - 1, z - 1] = part[x, y, z] + gathered(flat((x, y, z)))

    unrolled(n_own, 4, own_force)
    for plane in (1, 0):
        for n, region in enumerate(REGIONS):
            if region[0] == plane:
                back[region].wait()
                force_ref[edge_at(region, size)] += buffers[n][...]
    for p in range(len(sums)):
        for n, copy in enumerate(started):
            copy.wait()
            e = e + arrived[p][n]
        if p + 1 < len(sums):
            esum[p + 1] = e
            started = send_energy(p + 1)
    energy_ref[0, 0] = jnp.sum(e)


def on_device(coords, charges, atom_types, counts, c6_table, c12_table):
    cx, cy, cz, _, slots = coords.shape
    nt = c6_table.shape[0]
    size = (cx, cy, cz)
    n_ext = (cx + 1) * (cy + 2) * (cz + 2)
    n = cx * cy * cz
    f32 = jnp.float32
    bf = jnp.bfloat16
    vm = pl.BlockSpec(memory_space=pltpu.VMEM)
    sm = pl.BlockSpec(memory_space=pltpu.SMEM)
    grid = (cx + 1, cy + 2, cz + 2)
    sums = phases()
    most = max(len(members) for members in WITHIN + BEYOND)

    def extent(region):
        return tuple(s.size for s in edge_at(region, size)) + (3, slots)

    forces, energy = pl.pallas_call(
        functools.partial(pair_kernel, size, nt),
        out_shape=(
            jax.ShapeDtypeStruct(coords.shape, f32),
            jax.ShapeDtypeStruct((1, 1), f32),
        ),
        in_specs=[vm, vm, vm, sm, vm, vm],
        out_specs=(vm, sm),
        scratch_shapes=[
            pltpu.VMEM((*size, 8, slots), f32),
            pltpu.VMEM((*grid, 8, slots), f32),
            pltpu.VMEM((*grid, 3, slots), f32),
            pltpu.VMEM((n_ext, slots, slots), bf),
            pltpu.VMEM((n_ext, slots, FEATS), bf),
            pltpu.VMEM((n_ext, 8, slots), f32),
            pltpu.VMEM((n, slots, 2 * slots), bf),
            pltpu.VMEM((n, len(AXIS_SHIFTS) + 1, 8, slots), f32),
            pltpu.VMEM((n, 2 * slots, slots), bf),
            pltpu.VMEM((max(len(WITHIN), len(BEYOND)), most * slots, 2 * slots), bf),
            pltpu.VMEM((n_ext, slots, slots), f32),
            pltpu.VMEM((len(OFFSETS), 8, slots), f32),
            pltpu.VMEM((len(sums), 8, slots), f32),
            *(pltpu.VMEM(extent(region), f32) for region in REGIONS),
            *[pltpu.SemaphoreType.DMA((len(REGIONS),))] * 4,
            *(pltpu.VMEM((len(steps), 8, slots), f32) for steps in sums),
            *(pltpu.SemaphoreType.DMA((len(steps),)) for steps in sums for _ in range(2)),
        ],
        compiler_params=pltpu.CompilerParams(
            collective_id=0, has_side_effects=True, vmem_limit_bytes=56 * 2**20
        ),
    )(coords, charges, atom_types, counts, c6_table, c12_table)
    return forces, energy.reshape(1)


def solution(mesh):
    return jax.shard_map(
        on_device,
        mesh=mesh,
        in_specs=(
            P(("groups", "gx"), "gy", "gz", None, None),
            P(("groups", "gx"), "gy", "gz", None),
            P(("groups", "gx"), "gy", "gz", None),
            P(("groups", "gx"), "gy", "gz"),
            P(),
            P(),
        ),
        out_specs=(P(("groups", "gx"), "gy", "gz", None, None), P("groups")),
        check_vma=False,
    )
```

```python
import functools

import jax
import jax.numpy as jnp
from jax import lax
from jax.experimental import pallas as pl
from jax.experimental.pallas import tpu as pltpu
from jax.sharding import PartitionSpec as P

CELL_EDGE = 1.1
SOFTEN = 0.09
ENERGY_UNIT = 0.1
EDGE_V = 1.0 / (1.0 + SOFTEN)
E0 = EDGE_V**0.5
E3 = EDGE_V**3
STRIP = 32
TOGETHER = 4
WITHIN = ((0, 1, 2), (3, 13))
BEYOND = ((4, 5), (6, 7), (8, 9), (10, 11, 12))
OFFSETS = (
    (0, 0, 1), (0, 1, -1), (0, 1, 0), (0, 1, 1),
    (1, -1, -1), (1, -1, 0), (1, -1, 1),
    (1, 0, -1), (1, 0, 0), (1, 0, 1),
    (1, 1, -1), (1, 1, 0), (1, 1, 1), (0, 0, 0),
)
AXIS_SHIFTS = ((0, 0), (0, 1), (1, -1), (1, 0), (1, 1), (2, -1), (2, 0), (2, 1))
FEATS = 32


def rounded(value):
    return value.astype(jnp.bfloat16).astype(jnp.float32)


def two_parts(value):
    high = rounded(value)
    return high, rounded(value - high)


def three_parts(value):
    high = rounded(value)
    rest = value - high
    middle = rounded(rest)
    return high, middle, rounded(rest - middle)


def pick_rows(rows, choices):
    out = jnp.zeros(rows.shape, jnp.float32)
    for r, value in enumerate(choices):
        if value is not None:
            out = jnp.where(rows == r, value, out)
    return out


def dot(a, b):
    return jnp.dot(a, b, preferred_element_type=jnp.float32)


def unroll_of(count, most):
    return max(u for u in range(1, most + 1) if count % u == 0)


def unrolled(count, most, body):
    u = unroll_of(count, most)

    def step(i, carry):
        for k in range(u):
            body(i * u + k)
        return carry

    lax.fori_loop(0, count // u, step, 0)


MESH = pl.DeviceIdType.MESH
AXES = ("gx", "gy", "gz")
REGIONS = (
    (1, 0, 0), (1, 1, 0), (1, -1, 0), (1, 0, 1), (1, 0, -1), (1, 1, 1), (1, 1, -1), (1, -1, 1), (1, -1, -1),
    (0, 1, 0), (0, 1, 1), (0, 1, -1), (0, 0, 1), (0, 0, -1),
)


def sizes():
    return tuple(lax.axis_size(name) for name in AXES)


def device_at(step):
    return {name: lax.rem(lax.axis_index(name) + d % n, n) for name, d, n in zip(AXES, step, sizes())}


def wrapped(step):
    return tuple(d % n for d, n in zip(step, sizes()))


def greet(steps):
    barrier = pltpu.get_barrier_semaphore()
    near = {wrapped(s) for s in steps} | {wrapped([-d for d in s]) for s in steps}
    near = sorted(near - {(0, 0, 0)})
    for step in near:
        pl.semaphore_signal(barrier, inc=1, device_id=device_at(step), device_id_type=MESH)
    return len(near)


def halo_at(region, size):
    cx, cy, cz = size
    x = pl.ds(cx, 1) if region[0] else pl.ds(0, cx)
    y = {-1: pl.ds(0, 1), 0: pl.ds(1, cy), 1: pl.ds(cy + 1, 1)}[region[1]]
    z = {-1: pl.ds(0, 1), 0: pl.ds(1, cz), 1: pl.ds(cz + 1, 1)}[region[2]]
    return x, y, z


def edge_at(region, size):
    cx, cy, cz = size
    x = pl.ds(0, 1) if region[0] else pl.ds(0, cx)
    y = {-1: pl.ds(cy - 1, 1), 0: pl.ds(0, cy), 1: pl.ds(0, 1)}[region[1]]
    z = {-1: pl.ds(cz - 1, 1), 0: pl.ds(0, cz), 1: pl.ds(0, 1)}[region[2]]
    return x, y, z


def phases():
    nx, ny, nz = sizes()
    plane = [(0, y, z) for y in range(ny) for z in range(nz)]
    if nx * ny * nz <= 16:
        return ([(x, y, z) for x in range(nx) for _, y, z in plane][1:],)
    return plane[1:], [(x, 0, 0) for x in range(1, nx)]


def pair_kernel(size, nt, coords_ref, charge_ref, type_ref, count_ref, c6_ref, c12_ref, force_ref, energy_ref,
                local, ext, part, lh, lc, pos, wc, blocks, xi, gg, fb, fa, esum, *scratch):
    cx, cy, cz = size
    ey = cy + 2
    ez = cz + 2
    slots = 128
    n_ext = (cx + 1) * ey * ez
    n_own = cx * cy * cz
    bf = jnp.bfloat16
    buffers = scratch[: len(REGIONS)]
    send_sem, recv_sem, back_send, back_recv = scratch[len(REGIONS) : len(REGIONS) + 4]
    sums = phases()
    arrived = scratch[len(REGIONS) + 4 : len(REGIONS) + 4 + len(sums)]
    sum_sems = scratch[len(REGIONS) + 4 + len(sums) :]
    rows = lax.broadcasted_iota(jnp.int32, (8, slots), 0)
    lanes = lax.broadcasted_iota(jnp.int32, (1, slots), 1)
    ids = lax.broadcasted_iota(jnp.int32, (nt, slots), 0).astype(jnp.float32)
    one = jnp.ones((1, slots), jnp.float32)

    greeted = greet([*REGIONS, *(step for steps in sums for step in steps)])
    for x in range(cx):
        for y in range(cy):
            for z in range(cz):
                occupied = lanes < count_ref[x, y, z]
                charge = jnp.where(occupied, charge_ref[x, y, z : z + 1, :], 0.0)
                kind = jnp.where(occupied, type_ref[x, y, z : z + 1, :], nt).astype(jnp.float32)
                tile = jnp.concatenate([*(coords_ref[x, y, k, z : z + 1, :] for k in range(3)), charge, kind, jnp.zeros((3, slots), jnp.float32)], axis=0)
                local[x, y, z] = tile
                ext[x, y + 1, z + 1] = tile

    copies = {}
    for n, region in enumerate(REGIONS):
        copies[region] = pltpu.make_async_remote_copy(
            src_ref=local.at[edge_at(region, size)],
            dst_ref=ext.at[halo_at(region, size)],
            send_sem=send_sem.at[n],
            recv_sem=recv_sem.at[n],
            device_id=device_at([-d for d in region]),
            device_id_type=MESH,
        )
    c6 = c6_ref[...]
    c12 = c12_ref[...]
    c12 = (0.5 * ENERGY_UNIT) * (c12 + c12.T)
    c6 = (0.5 * ENERGY_UNIT) * (c6 + c6.T) - (2.0 * E3) * c12
    both = jnp.concatenate([c12, c6], axis=0)
    high = both.astype(bf)
    low = (both - high.astype(jnp.float32)).astype(bf)

    def flat(p):
        return (p[0] * ey + p[1]) * ez + p[2]

    def place(a):
        return a // (cy * cz), (a // cz) % cy + 1, a % cz + 1

    def prepare(p):
        c = flat(p)
        f = ext[p[0], p[1], p[2]]
        hot = (ids == f[4:5, :]).astype(jnp.float32).astype(bf)
        parts = [two_parts(f[k : k + 1, :] - 0.5 * CELL_EDGE) for k in range(3)]
        feats = []
        norm = None
        for h, m in parts:
            feats.append(pick_rows(rows, (h, h, m, m, one, one, one)))
            x = h + m
            norm = x * x if norm is None else norm + x * x
        qh, qm = two_parts(f[3:4, :])
        feats.append(pick_rows(rows, (*three_parts(norm), qh, qh, qm, qm)))
        (xh, xm), (yh, ym), (zh, zm) = parts
        pos[c] = pick_rows(rows, (xh, xm, yh, ym, zh, zm, one))
        lc[c] = jnp.concatenate(feats, axis=0).astype(bf).T
        lh[c] = jnp.concatenate([hot, hot], axis=0).T
        fb[c] = jnp.zeros((slots, slots), jnp.float32)

    def weights(a):
        x, y, z = place(a)
        f = ext[x, y, z]
        hot = (ids == f[4:5, :]).astype(jnp.float32).astype(bf)
        th = dot(high, hot).astype(bf)
        tl = dot(low, hot).astype(bf)
        wc[a, :, :slots] = jnp.concatenate([th[:nt], tl[:nt]], axis=0)
        wc[a, :, slots:] = jnp.concatenate([th[nt:], tl[nt:]], axis=0)
        for n, (k, shift) in enumerate(AXIS_SHIFTS):
            h, m = two_parts(f[k : k + 1, :] - (0.5 * CELL_EDGE + shift * CELL_EDGE))
            r = h + m
            sq = r * r
            if k == 0:
                sq = sq + SOFTEN
            h2 = -2.0 * h
            m2 = -2.0 * m
            blocks[a, n] = pick_rows(rows, (h2, m2, h2, m2, *three_parts(sq)))
        qh, qm = two_parts(ENERGY_UNIT * f[3:4, :])
        blocks[a, len(AXIS_SHIFTS)] = pick_rows(rows, (None, None, None, qh, qm, qh, qm))
        group = pos[flat((x, y, z))]
        xt = jnp.concatenate([group] * (slots // 8), axis=0).astype(bf).T
        xi[a] = jnp.concatenate([xt, xt], axis=0)

    norm_block = jnp.where(rows < 3, 1.0, 0.0)
    zero_block = jnp.zeros((8, slots), jnp.float32)
    strip_rows = lax.broadcasted_iota(jnp.int32, (STRIP, slots), 0)
    strip_lanes = lax.broadcasted_iota(jnp.int32, (STRIP, slots), 1)

    def own_index(p):
        return (p[0] * cy + p[1] - 1) * cz + p[2] - 1

    def neighbour(p, n):
        o = OFFSETS[n]
        return flat(p) + (o[0] * ey + o[1]) * ez + o[2]

    def forward(p, members):
        a = own_index(p)
        v1 = dot(jnp.concatenate([lh[neighbour(p, n)] for n in members], axis=0), wc[a])
        v2 = []
        charge = jnp.concatenate([zero_block] * 3 + [blocks[a, len(AXIS_SHIFTS)]], axis=0).astype(bf)
        for n in members:
            picks = [AXIS_SHIFTS.index((k, OFFSETS[n][k])) for k in range(3)]
            near = jnp.concatenate([blocks[a, k] for k in picks] + [norm_block], axis=0).astype(bf)
            v2.append(dot(lc[neighbour(p, n)], jnp.concatenate([near, charge], axis=1)))
        return v1, v2

    def compute(i, members, e_acc, vals):
        v1, v2 = vals
        for j, n in enumerate(members):
            own = OFFSETS[n] == (0, 0, 0)
            for r in range(0, slots, STRIP):
                at = pl.ds(j * slots + r, STRIP)
                t = v2[j][r : r + STRIP, :slots]
                charge = v2[j][r : r + STRIP, slots:]
                c12p = v1[j * slots + r : j * slots + r + STRIP, :slots]
                c6p = v1[j * slots + r : j * slots + r + STRIP, slots:]
                s = lax.rsqrt(t)
                v = s * s
                z3 = v * v * v
                w = jnp.maximum((1.0 + SOFTEN) - t, 0.0)
                if own:
                    w = jnp.where(strip_rows + r == strip_lanes, 0.0, w)
                y = z3 - E3
                m = c12p * y
                b1 = m - c6p
                u = y * b1 + charge * (s - E0)
                h = (z3 * (b1 + m)) * 6.0 + charge * s
                uw = u * w
                e = jnp.sum((uw * w).reshape(STRIP // 8, 8, slots), axis=0)
                e_acc = e_acc + (0.5 * e if own else e)
                g = w * (v * w * h) + 4.0 * uw
                gh = g.astype(bf)
                gg[i, at, :slots] = gh
                gg[i, at, slots:] = (g - gh.astype(jnp.float32)).astype(bf)
        return e_acc

    def spread(p, k, i, members):
        out = dot(gg[i, pl.ds(0, slots * len(members)), :], xi[own_index(p)])
        for j, n in enumerate(members):
            b = neighbour(p, n)
            if OFFSETS[n] != (0, 0, 0):
                fb[b, :, 8 * n : 8 * n + 8] = out[j * slots : (j + 1) * slots, 8 * n : 8 * n + 8]
            got = dot(pos[b].astype(bf), gg[i, pl.ds(j * slots, slots), :])
            fa[k, n] = got[:, :slots] + got[:, slots:]

    def shift_sum(parts):
        total = None
        extra = [zero_block] * 3
        for n, value in parts:
            total = value if total is None else total + value
            for k in range(3):
                o = OFFSETS[n][k]
                if o:
                    extra[k] = extra[k] + value if o > 0 else extra[k] - value
        return total, extra

    def force_of(c, parts, sign):
        total, extra = shift_sum(parts)
        x = pos[c]
        s = total[6:7]
        out = []
        for k in range(3):
            here = x[2 * k : 2 * k + 1] + x[2 * k + 1 : 2 * k + 2]
            moved = total[2 * k : 2 * k + 1] + total[2 * k + 1 : 2 * k + 2] + (sign * CELL_EDGE) * extra[k][6:7]
            out.append(here * s - moved)
        return jnp.concatenate(out, axis=0)

    def run(count, place_of, groups, e_acc):
        if not count:
            return e_acc
        names = [n for members in groups for n in members]
        cells = unroll_of(count, TOGETHER)
        plan = [(k, members) for k in range(cells) for members in groups]
        last = len(plan) - 1
        gg[last] = jnp.zeros(gg.shape[1:], bf)
        fa[...] = jnp.zeros(fa.shape, jnp.float32)

        def finish(p, k):
            part[p[0], p[1], p[2]] += force_of(flat(p), [(n, fa[k, n]) for n in names], 1.0)

        def cell(i, e_acc):
            places = [place_of(i * cells + k) for k in range(cells)]
            before = place_of((i * cells + count - 1) % count)
            vals = forward(places[0], groups[0])
            for m, (k, members) in enumerate(plan):
                ahead = forward(places[plan[m + 1][0]], plan[m + 1][1]) if m < last else None
                e_acc = compute(m, members, e_acc, vals)
                vals = ahead
                if m:
                    done, named = plan[m - 1]
                    spread(places[done], done, m - 1, named)
                    if done != k:
                        finish(places[done], done)
                else:
                    spread(before, cells - 1, last, groups[-1])
                    finish(before, cells - 1)
            return e_acc

        e_acc = lax.fori_loop(0, count // cells, cell, e_acc)
        spread(place_of(count - 1), cells - 1, last, groups[-1])
        finish(place_of(count - 1), cells - 1)
        return e_acc

    inner = (cy - 1) * (cz - 2)

    def inside(i):
        return i // inner, (i % inner) // (cz - 2) + 1, i % (cz - 2) + 2

    def at_sides(i):
        return i // (2 * (cy - 1)), (i // 2) % (cy - 1) + 1, (i % 2) * (cz - 1) + 1

    def at_top(i):
        return i // cz, cy, i % cz + 1

    def gathered(c):
        turned = fb[c].T
        return force_of(c, [(n, turned[8 * n : 8 * n + 8]) for n in range(len(OFFSETS) - 1)], -1.0)

    def gather(p):
        part[p[0], p[1], p[2]] = gathered(flat(p))

    def top_row(body):
        unrolled(cx * ez, 5, lambda i: body((i // ez, cy + 1, i % ez)))

    def side_columns(body):
        unrolled(2 * cx * cy, 4, lambda i: body((i // (2 * cy), (i // 2) % cy + 1, (i % 2) * (cz + 1))))

    def far_plane(body):
        unrolled(ey * ez, 5, lambda i: body((cx, i // ez, i % ez)))

    def send_back(plane):
        for n, region in enumerate(REGIONS):
            if region[0] == plane:
                back[region] = pltpu.make_async_remote_copy(
                    src_ref=part.at[halo_at(region, size)],
                    dst_ref=buffers[n],
                    send_sem=back_send.at[n],
                    recv_sem=back_recv.at[n],
                    device_id=device_at(region),
                    device_id_type=MESH,
                )
                back[region].start()

    def send_energy(p):
        started = []
        for n, step in enumerate(sums[p]):
            copy = pltpu.make_async_remote_copy(
                src_ref=esum.at[p],
                dst_ref=arrived[p].at[n],
                send_sem=sum_sems[2 * p].at[n],
                recv_sem=sum_sems[2 * p + 1].at[n],
                device_id=device_at(step),
                device_id_type=MESH,
            )
            copy.start()
            started.append(copy)
        return started

    back = {}
    unrolled(n_own, 4, lambda a: prepare(place(a)))
    unrolled(n_own, 4, weights)
    part[...] = jnp.zeros(part.shape, jnp.float32)
    early = cx * inner // 3
    e = run(early, inside, WITHIN, zero_block)
    pl.semaphore_wait(pltpu.get_barrier_semaphore(), greeted)
    for region in REGIONS:
        copies[region].start()
    e = run(cx * inner - early, lambda i: inside(i + early), WITHIN, e)
    for region in REGIONS:
        copies[region].wait()
    top_row(prepare)
    side_columns(prepare)
    far_plane(prepare)
    e = run(n_own, place, BEYOND, e)
    far_plane(gather)
    send_back(1)
    e = run(2 * cx * (cy - 1), at_sides, WITHIN, e)
    e = run(cx * cz, at_top, WITHIN, e)
    esum[0] = e
    top_row(gather)
    started = send_energy(0)
    side_columns(gather)
    send_back(0)

    def own_force(a):
        x, y, z = place(a)
        total = part[x, y, z] + gathered(flat((x, y, z)))
        for k in range(3):
            force_ref[x, y - 1, k, pl.ds(z - 1, 1), :] = total[k : k + 1]

    unrolled(n_own, 4, own_force)
    for plane in (1, 0):
        for n, region in enumerate(REGIONS):
            if region[0] == plane:
                back[region].wait()
                x, y, z = edge_at(region, size)
                for k in range(3):
                    force_ref[x, y, k, z, :] += buffers[n][:, :, :, k, :]
    for p in range(len(sums)):
        for n, copy in enumerate(started):
            copy.wait()
            e = e + arrived[p][n]
        if p + 1 < len(sums):
            esum[p + 1] = e
            started = send_energy(p + 1)
    energy_ref[0, 0] = jnp.sum(e)


def on_device(coords, charges, atom_types, counts, c6_table, c12_table):
    cx, cy, cz, _, slots = coords.shape
    nt = c6_table.shape[0]
    size = (cx, cy, cz)
    n_ext = (cx + 1) * (cy + 2) * (cz + 2)
    n = cx * cy * cz
    f32 = jnp.float32
    bf = jnp.bfloat16
    vm = pl.BlockSpec(memory_space=pltpu.VMEM)
    sm = pl.BlockSpec(memory_space=pltpu.SMEM)
    grid = (cx + 1, cy + 2, cz + 2)
    sums = phases()
    most = max(len(members) for members in WITHIN + BEYOND)

    def extent(region):
        return tuple(s.size for s in edge_at(region, size)) + (3, slots)

    forces, energy = pl.pallas_call(
        functools.partial(pair_kernel, size, nt),
        out_shape=(
            jax.ShapeDtypeStruct((cx, cy, 3, cz, slots), f32),
            jax.ShapeDtypeStruct((1, 1), f32),
        ),
        in_specs=[vm, vm, vm, sm, vm, vm],
        out_specs=(vm, sm),
        scratch_shapes=[
            pltpu.VMEM((*size, 8, slots), f32),
            pltpu.VMEM((*grid, 8, slots), f32),
            pltpu.VMEM((*grid, 3, slots), f32),
            pltpu.VMEM((n_ext, slots, slots), bf),
            pltpu.VMEM((n_ext, slots, FEATS), bf),
            pltpu.VMEM((n_ext, 8, slots), f32),
            pltpu.VMEM((n, slots, 2 * slots), bf),
            pltpu.VMEM((n, len(AXIS_SHIFTS) + 1, 8, slots), f32),
            pltpu.VMEM((n, 2 * slots, slots), bf),
            pltpu.VMEM((TOGETHER * max(len(WITHIN), len(BEYOND)), most * slots, 2 * slots), bf),
            pltpu.VMEM((n_ext, slots, slots), f32),
            pltpu.VMEM((TOGETHER, len(OFFSETS), 8, slots), f32),
            pltpu.VMEM((len(sums), 8, slots), f32),
            *(pltpu.VMEM(extent(region), f32) for region in REGIONS),
            *[pltpu.SemaphoreType.DMA((len(REGIONS),))] * 4,
            *(pltpu.VMEM((len(steps), 8, slots), f32) for steps in sums),
            *(pltpu.SemaphoreType.DMA((len(steps),)) for steps in sums for _ in range(2)),
        ],
        compiler_params=pltpu.CompilerParams(
            collective_id=0, has_side_effects=True, vmem_limit_bytes=56 * 2**20
        ),
    )(jnp.swapaxes(coords, 2, 3), charges, atom_types, counts, c6_table, c12_table)
    return jnp.swapaxes(forces, 2, 3), energy.reshape(1)


def solution(mesh):
    return jax.shard_map(
        on_device,
        mesh=mesh,
        in_specs=(
            P(("groups", "gx"), "gy", "gz", None, None),
            P(("groups", "gx"), "gy", "gz", None),
            P(("groups", "gx"), "gy", "gz", None),
            P(("groups", "gx"), "gy", "gz"),
            P(),
            P(),
        ),
        out_specs=(P(("groups", "gx"), "gy", "gz", None, None), P("groups")),
        check_vma=False,
    )
```

```python
import functools

import jax
import jax.numpy as jnp
from jax import lax
from jax.experimental import pallas as pl
from jax.experimental.pallas import tpu as pltpu
from jax.sharding import PartitionSpec as P

CELL_EDGE = 1.1
SOFTEN = 0.09
ENERGY_UNIT = 0.1
EDGE_V = 1.0 / (1.0 + SOFTEN)
E0 = EDGE_V**0.5
E3 = EDGE_V**3
STRIP = 128
TOGETHER = 4
WITHIN = ((0, 1, 2), (3, 13))
BEYOND = ((4, 5), (6, 7), (8, 9), (10, 11, 12))
OFFSETS = (
    (0, 0, 1), (0, 1, -1), (0, 1, 0), (0, 1, 1),
    (1, -1, -1), (1, -1, 0), (1, -1, 1),
    (1, 0, -1), (1, 0, 0), (1, 0, 1),
    (1, 1, -1), (1, 1, 0), (1, 1, 1), (0, 0, 0),
)
AXIS_SHIFTS = ((0, 0), (0, 1), (1, -1), (1, 0), (1, 1), (2, -1), (2, 0), (2, 1))
FEATS = 32


def rounded(value):
    return value.astype(jnp.bfloat16).astype(jnp.float32)


def two_parts(value):
    high = rounded(value)
    return high, rounded(value - high)


def three_parts(value):
    high = rounded(value)
    rest = value - high
    middle = rounded(rest)
    return high, middle, rounded(rest - middle)


def pick_rows(rows, choices):
    out = jnp.zeros(rows.shape, jnp.float32)
    for r, value in enumerate(choices):
        if value is not None:
            out = jnp.where(rows == r, value, out)
    return out


def dot(a, b):
    return jnp.dot(a, b, preferred_element_type=jnp.float32)


def unroll_of(count, most):
    return max(u for u in range(1, most + 1) if count % u == 0)


def unrolled(count, most, body):
    u = unroll_of(count, most)

    def step(i, carry):
        for k in range(u):
            body(i * u + k)
        return carry

    lax.fori_loop(0, count // u, step, 0)


MESH = pl.DeviceIdType.MESH
AXES = ("gx", "gy", "gz")
REGIONS = (
    (1, 0, 0), (1, 1, 0), (1, -1, 0), (1, 0, 1), (1, 0, -1), (1, 1, 1), (1, 1, -1), (1, -1, 1), (1, -1, -1),
    (0, 1, 0), (0, 1, 1), (0, 1, -1), (0, 0, 1), (0, 0, -1),
)


def sizes():
    return tuple(lax.axis_size(name) for name in AXES)


def device_at(step):
    return {name: lax.rem(lax.axis_index(name) + d % n, n) for name, d, n in zip(AXES, step, sizes())}


def wrapped(step):
    return tuple(d % n for d, n in zip(step, sizes()))


def greet(steps):
    barrier = pltpu.get_barrier_semaphore()
    near = {wrapped(s) for s in steps} | {wrapped([-d for d in s]) for s in steps}
    near = sorted(near - {(0, 0, 0)})
    for step in near:
        pl.semaphore_signal(barrier, inc=1, device_id=device_at(step), device_id_type=MESH)
    return len(near)


def halo_at(region, size):
    cx, cy, cz = size
    x = pl.ds(cx, 1) if region[0] else pl.ds(0, cx)
    y = {-1: pl.ds(0, 1), 0: pl.ds(1, cy), 1: pl.ds(cy + 1, 1)}[region[1]]
    z = {-1: pl.ds(0, 1), 0: pl.ds(1, cz), 1: pl.ds(cz + 1, 1)}[region[2]]
    return x, y, z


def edge_at(region, size):
    cx, cy, cz = size
    x = pl.ds(0, 1) if region[0] else pl.ds(0, cx)
    y = {-1: pl.ds(cy - 1, 1), 0: pl.ds(0, cy), 1: pl.ds(0, 1)}[region[1]]
    z = {-1: pl.ds(cz - 1, 1), 0: pl.ds(0, cz), 1: pl.ds(0, 1)}[region[2]]
    return x, y, z


def phases():
    nx, ny, nz = sizes()
    plane = [(0, y, z) for y in range(ny) for z in range(nz)]
    if nx * ny * nz <= 16:
        return ([(x, y, z) for x in range(nx) for _, y, z in plane][1:],)
    return plane[1:], [(x, 0, 0) for x in range(1, nx)]


def pair_kernel(size, nt, coords_ref, charge_ref, type_ref, count_ref, c6_ref, c12_ref, force_ref, energy_ref,
                local, ext, part, lh, lc, pos, wc, blocks, xi, gg, fb, fa, esum, *scratch):
    cx, cy, cz = size
    ey = cy + 2
    ez = cz + 2
    slots = 128
    n_ext = (cx + 1) * ey * ez
    n_own = cx * cy * cz
    bf = jnp.bfloat16
    buffers = scratch[: len(REGIONS)]
    send_sem, recv_sem, back_send, back_recv = scratch[len(REGIONS) : len(REGIONS) + 4]
    sums = phases()
    arrived = scratch[len(REGIONS) + 4 : len(REGIONS) + 4 + len(sums)]
    sum_sems = scratch[len(REGIONS) + 4 + len(sums) :]
    rows = lax.broadcasted_iota(jnp.int32, (8, slots), 0)
    lanes = lax.broadcasted_iota(jnp.int32, (1, slots), 1)
    ids = lax.broadcasted_iota(jnp.int32, (nt, slots), 0).astype(jnp.float32)
    one = jnp.ones((1, slots), jnp.float32)

    greeted = greet([*REGIONS, *(step for steps in sums for step in steps)])
    for x in range(cx):
        for y in range(cy):
            for z in range(cz):
                occupied = lanes < count_ref[x, y, z]
                charge = jnp.where(occupied, charge_ref[x, y, z : z + 1, :], 0.0)
                kind = jnp.where(occupied, type_ref[x, y, z : z + 1, :], nt).astype(jnp.float32)
                tile = jnp.concatenate([*(coords_ref[x, y, k, z : z + 1, :] for k in range(3)), charge, kind, jnp.zeros((3, slots), jnp.float32)], axis=0)
                local[x, y, z] = tile
                ext[x, y + 1, z + 1] = tile

    copies = {}
    for n, region in enumerate(REGIONS):
        copies[region] = pltpu.make_async_remote_copy(
            src_ref=local.at[edge_at(region, size)],
            dst_ref=ext.at[halo_at(region, size)],
            send_sem=send_sem.at[n],
            recv_sem=recv_sem.at[n],
            device_id=device_at([-d for d in region]),
            device_id_type=MESH,
        )
    c6 = c6_ref[...]
    c12 = c12_ref[...]
    c12 = (0.5 * ENERGY_UNIT) * (c12 + c12.T)
    c6 = (0.5 * ENERGY_UNIT) * (c6 + c6.T) - (2.0 * E3) * c12
    both = jnp.concatenate([c12, c6], axis=0)
    high = both.astype(bf)
    low = (both - high.astype(jnp.float32)).astype(bf)

    def flat(p):
        return (p[0] * ey + p[1]) * ez + p[2]

    def place(a):
        return a // (cy * cz), (a // cz) % cy + 1, a % cz + 1

    def prepare(p):
        c = flat(p)
        f = ext[p[0], p[1], p[2]]
        hot = (ids == f[4:5, :]).astype(jnp.float32).astype(bf)
        parts = [two_parts(f[k : k + 1, :] - 0.5 * CELL_EDGE) for k in range(3)]
        feats = []
        norm = None
        for h, m in parts:
            feats.append(pick_rows(rows, (h, h, m, m, one, one, one)))
            x = h + m
            norm = x * x if norm is None else norm + x * x
        qh, qm = two_parts(f[3:4, :])
        feats.append(pick_rows(rows, (*three_parts(norm), qh, qh, qm, qm)))
        (xh, xm), (yh, ym), (zh, zm) = parts
        pos[c] = pick_rows(rows, (xh, xm, yh, ym, zh, zm, one))
        lc[c] = jnp.concatenate(feats, axis=0).astype(bf).T
        lh[c] = jnp.concatenate([hot, hot], axis=0).T
        fb[c] = jnp.zeros((slots, slots), jnp.float32)

    def weights(a):
        x, y, z = place(a)
        f = ext[x, y, z]
        hot = (ids == f[4:5, :]).astype(jnp.float32).astype(bf)
        th = dot(high, hot).astype(bf)
        tl = dot(low, hot).astype(bf)
        wc[a, :, :slots] = jnp.concatenate([th[:nt], tl[:nt]], axis=0)
        wc[a, :, slots:] = jnp.concatenate([th[nt:], tl[nt:]], axis=0)
        for n, (k, shift) in enumerate(AXIS_SHIFTS):
            h, m = two_parts(f[k : k + 1, :] - (0.5 * CELL_EDGE + shift * CELL_EDGE))
            r = h + m
            sq = r * r
            if k == 0:
                sq = sq + SOFTEN
            h2 = -2.0 * h
            m2 = -2.0 * m
            blocks[a, n] = pick_rows(rows, (h2, m2, h2, m2, *three_parts(sq)))
        qh, qm = two_parts(ENERGY_UNIT * f[3:4, :])
        blocks[a, len(AXIS_SHIFTS)] = pick_rows(rows, (None, None, None, qh, qm, qh, qm))
        group = pos[flat((x, y, z))]
        xt = jnp.concatenate([group] * (slots // 8), axis=0).astype(bf).T
        xi[a] = jnp.concatenate([xt, xt], axis=0)

    norm_block = jnp.where(rows < 3, 1.0, 0.0)
    zero_block = jnp.zeros((8, slots), jnp.float32)
    strip_rows = lax.broadcasted_iota(jnp.int32, (STRIP, slots), 0)
    strip_lanes = lax.broadcasted_iota(jnp.int32, (STRIP, slots), 1)

    def own_index(p):
        return (p[0] * cy + p[1] - 1) * cz + p[2] - 1

    def neighbour(p, n):
        o = OFFSETS[n]
        return flat(p) + (o[0] * ey + o[1]) * ez + o[2]

    def forward(p, members):
        a = own_index(p)
        v1 = dot(jnp.concatenate([lh[neighbour(p, n)] for n in members], axis=0), wc[a])
        v2 = []
        charge = jnp.concatenate([zero_block] * 3 + [blocks[a, len(AXIS_SHIFTS)]], axis=0).astype(bf)
        for n in members:
            picks = [AXIS_SHIFTS.index((k, OFFSETS[n][k])) for k in range(3)]
            near = jnp.concatenate([blocks[a, k] for k in picks] + [norm_block], axis=0).astype(bf)
            v2.append(dot(lc[neighbour(p, n)], jnp.concatenate([near, charge], axis=1)))
        return v1, v2

    def compute(i, members, e_acc, vals):
        v1, v2 = vals
        for j, n in enumerate(members):
            own = OFFSETS[n] == (0, 0, 0)
            for r in range(0, slots, STRIP):
                at = pl.ds(j * slots + r, STRIP)
                t = v2[j][r : r + STRIP, :slots]
                charge = v2[j][r : r + STRIP, slots:]
                c12p = v1[j * slots + r : j * slots + r + STRIP, :slots]
                c6p = v1[j * slots + r : j * slots + r + STRIP, slots:]
                s = lax.rsqrt(t)
                v = s * s
                z3 = v * v * v
                w = jnp.maximum((1.0 + SOFTEN) - t, 0.0)
                if own:
                    w = jnp.where(strip_rows + r == strip_lanes, 0.0, w)
                y = z3 - E3
                m = c12p * y
                b1 = m - c6p
                u = y * b1 + charge * (s - E0)
                h = (z3 * (b1 + m)) * 6.0 + charge * s
                uw = u * w
                e = jnp.sum((uw * w).reshape(STRIP // 8, 8, slots), axis=0)
                e_acc = e_acc + (0.5 * e if own else e)
                g = w * (v * w * h) + 4.0 * uw
                gh = g.astype(bf)
                gg[i, at, :slots] = gh
                gg[i, at, slots:] = (g - gh.astype(jnp.float32)).astype(bf)
        return e_acc

    def spread(p, k, i, members):
        out = dot(gg[i, pl.ds(0, slots * len(members)), :], xi[own_index(p)])
        for j, n in enumerate(members):
            b = neighbour(p, n)
            if OFFSETS[n] != (0, 0, 0):
                fb[b, :, 8 * n : 8 * n + 8] = out[j * slots : (j + 1) * slots, 8 * n : 8 * n + 8]
            got = dot(pos[b].astype(bf), gg[i, pl.ds(j * slots, slots), :])
            fa[k, n] = got[:, :slots] + got[:, slots:]

    def shift_sum(parts):
        total = None
        extra = [zero_block] * 3
        for n, value in parts:
            total = value if total is None else total + value
            for k in range(3):
                o = OFFSETS[n][k]
                if o:
                    extra[k] = extra[k] + value if o > 0 else extra[k] - value
        return total, extra

    def force_of(c, parts, sign):
        total, extra = shift_sum(parts)
        x = pos[c]
        s = total[6:7]
        out = []
        for k in range(3):
            here = x[2 * k : 2 * k + 1] + x[2 * k + 1 : 2 * k + 2]
            moved = total[2 * k : 2 * k + 1] + total[2 * k + 1 : 2 * k + 2] + (sign * CELL_EDGE) * extra[k][6:7]
            out.append(here * s - moved)
        return jnp.concatenate(out, axis=0)

    def run(count, place_of, groups, e_acc):
        if not count:
            return e_acc
        names = [n for members in groups for n in members]
        cells = unroll_of(count, TOGETHER)
        plan = [(k, members) for k in range(cells) for members in groups]
        last = len(plan) - 1
        gg[last] = jnp.zeros(gg.shape[1:], bf)
        fa[...] = jnp.zeros(fa.shape, jnp.float32)

        def finish(p, k):
            part[p[0], p[1], p[2]] += force_of(flat(p), [(n, fa[k, n]) for n in names], 1.0)

        def cell(i, e_acc):
            places = [place_of(i * cells + k) for k in range(cells)]
            before = place_of((i * cells + count - 1) % count)
            vals = forward(places[0], groups[0])
            for m, (k, members) in enumerate(plan):
                ahead = forward(places[plan[m + 1][0]], plan[m + 1][1]) if m < last else None
                e_acc = compute(m, members, e_acc, vals)
                vals = ahead
                if m:
                    done, named = plan[m - 1]
                    spread(places[done], done, m - 1, named)
                    if done != k:
                        finish(places[done], done)
                else:
                    spread(before, cells - 1, last, groups[-1])
                    finish(before, cells - 1)
            return e_acc

        e_acc = lax.fori_loop(0, count // cells, cell, e_acc)
        spread(place_of(count - 1), cells - 1, last, groups[-1])
        finish(place_of(count - 1), cells - 1)
        return e_acc

    inner = (cy - 1) * (cz - 2)

    def inside(i):
        return i // inner, (i % inner) // (cz - 2) + 1, i % (cz - 2) + 2

    def at_sides(i):
        return i // (2 * (cy - 1)), (i // 2) % (cy - 1) + 1, (i % 2) * (cz - 1) + 1

    def at_top(i):
        return i // cz, cy, i % cz + 1

    def gathered(c):
        turned = fb[c].T
        return force_of(c, [(n, turned[8 * n : 8 * n + 8]) for n in range(len(OFFSETS) - 1)], -1.0)

    def gather(p):
        part[p[0], p[1], p[2]] = gathered(flat(p))

    def top_row(body):
        unrolled(cx * ez, 10, lambda i: body((i // ez, cy + 1, i % ez)))

    def side_columns(body):
        unrolled(2 * cx * cy, 8, lambda i: body((i // (2 * cy), (i // 2) % cy + 1, (i % 2) * (cz + 1))))

    def far_plane(body):
        unrolled(ey * ez, 10, lambda i: body((cx, i // ez, i % ez)))

    def send_back(plane):
        for n, region in enumerate(REGIONS):
            if region[0] == plane:
                back[region] = pltpu.make_async_remote_copy(
                    src_ref=part.at[halo_at(region, size)],
                    dst_ref=buffers[n],
                    send_sem=back_send.at[n],
                    recv_sem=back_recv.at[n],
                    device_id=device_at(region),
                    device_id_type=MESH,
                )
                back[region].start()

    def send_energy(p):
        started = []
        for n, step in enumerate(sums[p]):
            copy = pltpu.make_async_remote_copy(
                src_ref=esum.at[p],
                dst_ref=arrived[p].at[n],
                send_sem=sum_sems[2 * p].at[n],
                recv_sem=sum_sems[2 * p + 1].at[n],
                device_id=device_at(step),
                device_id_type=MESH,
            )
            copy.start()
            started.append(copy)
        return started

    back = {}
    unrolled(n_own, 8, lambda a: prepare(place(a)))
    unrolled(n_own, 4, weights)
    part[...] = jnp.zeros(part.shape, jnp.float32)
    early = cx * inner // 3
    e = run(early, inside, WITHIN, zero_block)
    pl.semaphore_wait(pltpu.get_barrier_semaphore(), greeted)
    for region in REGIONS:
        copies[region].start()
    e = run(cx * inner - early, lambda i: inside(i + early), WITHIN, e)
    for region in REGIONS:
        copies[region].wait()
    top_row(prepare)
    side_columns(prepare)
    far_plane(prepare)
    e = run(n_own, place, BEYOND, e)
    far_plane(gather)
    send_back(1)
    e = run(2 * cx * (cy - 1), at_sides, WITHIN, e)
    e = run(cx * cz, at_top, WITHIN, e)
    esum[0] = e
    top_row(gather)
    started = send_energy(0)
    side_columns(gather)
    send_back(0)

    def own_force(a):
        x, y, z = place(a)
        total = part[x, y, z] + gathered(flat((x, y, z)))
        for k in range(3):
            force_ref[x, y - 1, k, pl.ds(z - 1, 1), :] = -total[k : k + 1]

    unrolled(n_own, 8, own_force)
    for plane in (1, 0):
        for n, region in enumerate(REGIONS):
            if region[0] == plane:
                back[region].wait()
                x, y, z = edge_at(region, size)
                for k in range(3):
                    force_ref[x, y, k, z, :] -= buffers[n][:, :, :, k, :]
    for p in range(len(sums)):
        for n, copy in enumerate(started):
            copy.wait()
            e = e + arrived[p][n]
        if p + 1 < len(sums):
            esum[p + 1] = e
            started = send_energy(p + 1)
    energy_ref[0, 0] = jnp.sum(e)


def on_device(coords, charges, atom_types, counts, c6_table, c12_table):
    cx, cy, cz, _, slots = coords.shape
    nt = c6_table.shape[0]
    size = (cx, cy, cz)
    n_ext = (cx + 1) * (cy + 2) * (cz + 2)
    n = cx * cy * cz
    f32 = jnp.float32
    bf = jnp.bfloat16
    vm = pl.BlockSpec(memory_space=pltpu.VMEM)
    sm = pl.BlockSpec(memory_space=pltpu.SMEM)
    grid = (cx + 1, cy + 2, cz + 2)
    sums = phases()
    most = max(len(members) for members in WITHIN + BEYOND)

    def extent(region):
        return tuple(s.size for s in edge_at(region, size)) + (3, slots)

    forces, energy = pl.pallas_call(
        functools.partial(pair_kernel, size, nt),
        out_shape=(
            jax.ShapeDtypeStruct((cx, cy, 3, cz, slots), f32),
            jax.ShapeDtypeStruct((1, 1), f32),
        ),
        in_specs=[vm, vm, vm, sm, vm, vm],
        out_specs=(vm, sm),
        scratch_shapes=[
            pltpu.VMEM((*size, 8, slots), f32),
            pltpu.VMEM((*grid, 8, slots), f32),
            pltpu.VMEM((*grid, 3, slots), f32),
            pltpu.VMEM((n_ext, slots, slots), bf),
            pltpu.VMEM((n_ext, slots, FEATS), bf),
            pltpu.VMEM((n_ext, 8, slots), f32),
            pltpu.VMEM((n, slots, 2 * slots), bf),
            pltpu.VMEM((n, len(AXIS_SHIFTS) + 1, 8, slots), f32),
            pltpu.VMEM((n, 2 * slots, slots), bf),
            pltpu.VMEM((TOGETHER * max(len(WITHIN), len(BEYOND)), most * slots, 2 * slots), bf),
            pltpu.VMEM((n_ext, slots, slots), f32),
            pltpu.VMEM((TOGETHER, len(OFFSETS), 8, slots), f32),
            pltpu.VMEM((len(sums), 8, slots), f32),
            *(pltpu.VMEM(extent(region), f32) for region in REGIONS),
            *[pltpu.SemaphoreType.DMA((len(REGIONS),))] * 4,
            *(pltpu.VMEM((len(steps), 8, slots), f32) for steps in sums),
            *(pltpu.SemaphoreType.DMA((len(steps),)) for steps in sums for _ in range(2)),
        ],
        compiler_params=pltpu.CompilerParams(
            collective_id=0, has_side_effects=True, vmem_limit_bytes=56 * 2**20
        ),
    )(jnp.swapaxes(coords, 2, 3), charges, atom_types, counts, c6_table, c12_table)
    return -jnp.swapaxes(forces, 2, 3), energy.reshape(1)


def solution(mesh):
    return jax.shard_map(
        on_device,
        mesh=mesh,
        in_specs=(
            P(("groups", "gx"), "gy", "gz", None, None),
            P(("groups", "gx"), "gy", "gz", None),
            P(("groups", "gx"), "gy", "gz", None),
            P(("groups", "gx"), "gy", "gz"),
            P(),
            P(),
        ),
        out_specs=(P(("groups", "gx"), "gy", "gz", None, None), P("groups")),
        check_vma=False,
    )
```
